32 devices in a mesh: gx: 8 (over z, y), gy: 4 (over x, core).
Axes of the slice: x: 2, y: 2, z: 4, core: 2. Of those that a mesh axis runs over, the one named last changes fastest.
Arguments:
- electric: float32 [3, 128, 512, 128], P(None, 'gx', 'gy'), may hold values from -6 to 6
- magnetic: float32 [3, 128, 512, 128], P(None, 'gx', 'gy'), may hold values from -6 to 6
- retention: float32 [128, 512, 128], P('gx', 'gy'), may hold values from 0.5 to 1
- coupling: float32 [128, 512, 128], P('gx', 'gy'), may hold values from 0.1 to 0.5
- spectrum_real: float32 [4, 4, 128, 512], P(None, None, 'gx', 'gy'), may hold values from -6 to 6
- spectrum_imag: float32 [4, 4, 128, 512], P(None, None, 'gx', 'gy'), may hold values from -6 to 6
- phases: float32 [4], replicated, may hold values from -3.140625 to 3.140625
Outputs:
- next_electric: float32 [3, 128, 512, 128], P(None, 'gx', 'gy')
- next_magnetic: float32 [3, 128, 512, 128], P(None, 'gx', 'gy')
- next_real: float32 [4, 4, 128, 512], P(None, None, 'gx', 'gy')
- next_imag: float32 [4, 4, 128, 512], P(None, None, 'gx', 'gy')
- far_field: float32 [2, 4, 4, 256, 256], P(None, None, None, 'gx', 'gy')
The draws below stay inside these ranges and needn't reach their ends.
All inputs are finite; a program needn't handle non-finite values.
Results may differ from the reference program's by a relative error of at most 0.000071.
Values sent between devices are 32-bit elements; how exact they have to be, the bound alone decides.
No kernel may reach another device: no remote copies, remote signals or barrier semaphores. Data moves between devices by JAX's collectives and lax.ppermute only.
A program may use at most 128 MiB of HBM per device.

```python
import math
import jax
import jax.numpy as jnp
from jax import lax

NZ = 128
FREQS = 4
WAVES = 256
TOP_PLANE = 111
NX = 128
NY = 512


def level_of(key, dims, split, smallest, high):
    loudness = 1.0
    for axis_at, blocks in split:
        draws = jax.random.uniform(jax.random.fold_in(jax.random.fold_in(key, 6), axis_at), (blocks,), jnp.float32, smallest / len(split), high / len(split))
        loudness = loudness * jnp.repeat(jnp.exp(draws), dims[axis_at] // blocks).reshape((-1,) + (1,) * (len(dims) - 1 - axis_at))
    return loudness


def noise(key, shape, width, most, split=(), kind=jnp.bfloat16):
    values = width * jax.random.normal(key, shape, jnp.float32)
    if split:
        values = values * level_of(key, shape, split, -0.22, 0.18)
    return jnp.clip(values, -most, most).astype(kind)


def setup_inputs(seed: int = 0) -> dict:
    key_list = jax.random.split(jax.random.key(seed), 8)
    return {
        "electric": noise(key_list[0], (3, NX, NY, NZ), 1.0, 6.0, ((1, 8), (2, 4)), jnp.float32),
        "magnetic": noise(key_list[1], (3, NX, NY, NZ), 1.0, 6.0, ((1, 8), (2, 4)), jnp.float32),
        "retention": jnp.clip(0.5 + 0.5 * jax.random.uniform(key_list[2], (NX, NY, NZ), jnp.float32) ** level_of(key_list[2], (NX, NY, NZ), ((0, 8), (1, 4)), -0.2, 0.2), 0.5, 1.0),
        "coupling": jnp.clip(jnp.exp(math.log(0.5) - 1.609438 * jax.random.uniform(key_list[3], (NX, NY, NZ), jnp.float32) ** level_of(key_list[3], (NX, NY, NZ), ((0, 8), (1, 4)), -0.2, 0.2)), 0.1, 0.5),
        "spectrum_real": noise(key_list[4], (4, FREQS, NX, NY), 1.0, 6.0, ((2, 8), (3, 4)), jnp.float32),
        "spectrum_imag": noise(key_list[5], (4, FREQS, NX, NY), 1.0, 6.0, ((2, 8), (3, 4)), jnp.float32),
        "phases": jnp.clip(jax.random.uniform(key_list[6], (FREQS,), jnp.float32, -3.140625, 3.140625), -3.140625, 3.140625),
    }


curl_step = 0.5

def forward_diff(values, along):
    padded = jnp.pad(values, [(0, 1) if which == along else (0, 0) for which in range(values.ndim)])
    return lax.slice_in_dim(padded, 1, values.shape[along] + 1, axis=along) - values

def backward_diff(values, along):
    padded = jnp.pad(values, [(1, 0) if which == along else (0, 0) for which in range(values.ndim)])
    return values - lax.slice_in_dim(padded, 0, values.shape[along], axis=along)

def tables(number, extent, offset):
    wave = 2 * jnp.arange(number, dtype=jnp.int32) + 1 - number
    places = offset + jnp.arange(extent, dtype=jnp.int32)
    folded = wave[:, None] * places[None, :] % (4 * number)
    angles = folded.astype(jnp.float32) * (math.pi / (2 * number))
    return (jnp.cos(angles), jnp.sin(angles))

def reference(electric, magnetic, retention, coupling, spectrum_real, spectrum_imag, phases):
    highest = lax.Precision.HIGHEST
    elec_x, elec_y, elec_z = (electric[0], electric[1], electric[2])
    mag_x = magnetic[0] - curl_step * (forward_diff(elec_z, 1) - forward_diff(elec_y, 2))
    mag_y = magnetic[1] - curl_step * (forward_diff(elec_x, 2) - forward_diff(elec_z, 0))
    mag_z = magnetic[2] - curl_step * (forward_diff(elec_y, 0) - forward_diff(elec_x, 1))
    new_x = retention * elec_x + coupling * (backward_diff(mag_z, 1) - backward_diff(mag_y, 2))
    new_y = retention * elec_y + coupling * (backward_diff(mag_x, 2) - backward_diff(mag_z, 0))
    new_z = retention * elec_z + coupling * (backward_diff(mag_y, 0) - backward_diff(mag_x, 1))
    tangent = jnp.stack([new_x[:, :, TOP_PLANE], new_y[:, :, TOP_PLANE], mag_x[:, :, TOP_PLANE], mag_y[:, :, TOP_PLANE]])
    next_real = spectrum_real + tangent[:, None] * jnp.cos(phases)[None, :, None, None]
    next_imag = spectrum_imag - tangent[:, None] * jnp.sin(phases)[None, :, None, None]
    cos_x, sin_x = tables(WAVES, NX, 0)
    cos_y, sin_y = tables(WAVES, NY, 0)
    part_real = jnp.einsum('cfxy,ky->cfxk', next_real, cos_y, precision=highest) + jnp.einsum('cfxy,ky->cfxk', next_imag, sin_y, precision=highest)
    part_imag = jnp.einsum('cfxy,ky->cfxk', next_imag, cos_y, precision=highest) - jnp.einsum('cfxy,ky->cfxk', next_real, sin_y, precision=highest)
    far_real = jnp.einsum('jx,cfxk->cfjk', cos_x, part_real, precision=highest) + jnp.einsum('jx,cfxk->cfjk', sin_x, part_imag, precision=highest)
    far_imag = jnp.einsum('jx,cfxk->cfjk', cos_x, part_imag, precision=highest) - jnp.einsum('jx,cfxk->cfjk', sin_x, part_real, precision=highest)
    scale = 1.0 / math.sqrt(NX * NY)
    far_field = jnp.stack([far_real, far_imag]) * scale
    next_electric = jnp.stack([new_x, new_y, new_z])
    next_magnetic = jnp.stack([mag_x, mag_y, mag_z])
    return (next_electric, next_magnetic, next_real, next_imag, far_field)
```

```python
import math

import jax
import jax.numpy as jnp
import numpy as np
from jax import lax
from jax.sharding import PartitionSpec as P

WAVES = 256
TOP_PLANE = 111
BOTH = ("gx", "gy")


curl_step = 0.5


def passed_along(value, axis, by):
    devices = lax.axis_size(axis)
    pairs = [(i, i + by) for i in range(devices) if 0 <= i + by < devices]
    return lax.ppermute(value, axis, pairs)


def forward_diff(values, along):
    padded = jnp.pad(values, [(0, 1) if which == along else (0, 0) for which in range(values.ndim)])
    return lax.slice_in_dim(padded, 1, values.shape[along] + 1, axis=along) - values


def backward_diff(values, along):
    padded = jnp.pad(values, [(1, 0) if which == along else (0, 0) for which in range(values.ndim)])
    return values - lax.slice_in_dim(padded, 0, values.shape[along], axis=along)


def ahead_diff(values, border, along):
    upper = lax.slice_in_dim(values, 1, values.shape[along], axis=along)
    return jnp.concatenate([upper, border], axis=along) - values


def behind_diff(values, border, along):
    lower = lax.slice_in_dim(values, 0, values.shape[along] - 1, axis=along)
    return values - jnp.concatenate([border, lower], axis=along)


def wave_tables(number, extent):
    wave = 2 * np.arange(number) + 1 - number
    angles = (wave[:, None] * np.arange(extent)[None, :] % (4 * number)) * (math.pi / (2 * number))
    return np.cos(angles).astype(np.float32), np.sin(angles).astype(np.float32)


def swapped(value, by):
    devices = lax.axis_size(BOTH)
    return lax.ppermute(value, BOTH, [(i, i ^ by) for i in range(devices)])


def far_of(next_real, next_imag):
    highest = lax.Precision.HIGHEST
    comps, freqs, rows, cols = next_real.shape
    along_x, along_y = lax.axis_size("gx"), lax.axis_size("gy")
    devices = along_x * along_y
    planes = comps * freqs
    share = devices // planes
    part_rows = rows // share
    wide = WAVES // along_y
    part_wide = wide // share
    tall = WAVES // along_x
    place = lax.axis_index(BOTH) % share

    both = jnp.stack([next_real, next_imag]).reshape(2, planes, share, part_rows, cols)
    both = both.transpose(1, 2, 0, 3, 4).reshape(devices, 2, part_rows, cols)
    got = lax.all_to_all(both, BOTH, split_axis=0, concat_axis=0, tiled=True)
    got = got.reshape(along_x, along_y, 2, part_rows, cols)

    cos_y, sin_y = wave_tables(WAVES, cols * along_y)
    order_k = np.arange(WAVES).reshape(along_y, share, part_wide).transpose(1, 0, 2).reshape(-1)
    cos_y = cos_y[order_k].reshape(share, -1, along_y, cols)
    sin_y = sin_y[order_k].reshape(share, -1, along_y, cols)
    with_cos = jnp.einsum("gbirc,skbc->sigrk", got, cos_y, precision=highest)
    with_sin = jnp.einsum("gbirc,skbc->sigrk", got, sin_y, precision=highest)
    partial = jnp.stack([with_cos[:, 0] + with_sin[:, 1], with_cos[:, 1] - with_sin[:, 0]], axis=1)

    pieces = []
    for by in range(share):
        piece = lax.dynamic_index_in_dim(partial, place ^ by, 0, keepdims=False)
        pieces.append(piece if by == 0 else swapped(piece, by))
    partial = jnp.stack([lax.dynamic_index_in_dim(jnp.stack(pieces), place ^ s, 0, keepdims=False) for s in range(share)])

    cos_x, sin_x = wave_tables(WAVES, rows * along_x)
    cos_x = cos_x.reshape(WAVES, along_x, share, part_rows)
    sin_x = sin_x.reshape(WAVES, along_x, share, part_rows)
    with_cos = jnp.einsum("jgsr,sigrk->ijk", cos_x, partial, precision=highest)
    with_sin = jnp.einsum("jgsr,sigrk->ijk", sin_x, partial, precision=highest)
    far = jnp.stack([with_cos[0] + with_sin[1], with_cos[1] - with_sin[0]])
    far = far * (1.0 / math.sqrt(rows * along_x * cols * along_y))

    far = far.reshape(2, along_x, tall, along_y, part_wide).transpose(1, 3, 0, 2, 4)
    far = far.reshape(devices, 2, tall, part_wide)
    far = lax.all_to_all(far, BOTH, split_axis=0, concat_axis=0, tiled=True)
    far = far.reshape(comps, freqs, share, 2, tall, part_wide).transpose(3, 0, 1, 4, 2, 5)
    return far.reshape(2, comps, freqs, tall, wide)


def per_device(electric, magnetic, retention, coupling, spectrum_real, spectrum_imag, phases):
    elec_x, elec_y, elec_z = (electric[0], electric[1], electric[2])
    rows_elec = passed_along(electric[1:3, 0:1], "gx", -1)
    cols_elec = passed_along(electric[0:3:2, :, 0:1], "gy", -1)
    mag_x = magnetic[0] - curl_step * (
        ahead_diff(elec_z, cols_elec[1], 1) - forward_diff(elec_y, 2)
    )
    mag_y = magnetic[1] - curl_step * (
        forward_diff(elec_x, 2) - ahead_diff(elec_z, rows_elec[1], 0)
    )
    mag_z = magnetic[2] - curl_step * (
        ahead_diff(elec_y, rows_elec[0], 0) - ahead_diff(elec_x, cols_elec[0], 1)
    )
    next_magnetic = jnp.stack([mag_x, mag_y, mag_z])
    rows_magn = passed_along(next_magnetic[1:3, -1:], "gx", 1)
    cols_magn = passed_along(next_magnetic[0:3:2, :, -1:], "gy", 1)
    new_x = retention * elec_x + coupling * (
        behind_diff(mag_z, cols_magn[1], 1) - backward_diff(mag_y, 2)
    )
    new_y = retention * elec_y + coupling * (
        backward_diff(mag_x, 2) - behind_diff(mag_z, rows_magn[1], 0)
    )
    new_z = retention * elec_z + coupling * (
        behind_diff(mag_y, rows_magn[0], 0) - behind_diff(mag_x, cols_magn[0], 1)
    )
    next_electric = jnp.stack([new_x, new_y, new_z])
    tangent = jnp.stack(
        [
            new_x[:, :, TOP_PLANE],
            new_y[:, :, TOP_PLANE],
            mag_x[:, :, TOP_PLANE],
            mag_y[:, :, TOP_PLANE],
        ]
    )
    next_real = spectrum_real + tangent[:, None] * jnp.cos(phases)[None, :, None, None]
    next_imag = spectrum_imag - tangent[:, None] * jnp.sin(phases)[None, :, None, None]
    far_field = far_of(next_real, next_imag)
    return (next_electric, next_magnetic, next_real, next_imag, far_field)


def solution(mesh):
    placed = (
        P(None, "gx", "gy", None),
        P(None, "gx", "gy", None),
        P("gx", "gy", None),
        P("gx", "gy", None),
        P(None, None, "gx", "gy"),
        P(None, None, "gx", "gy"),
        P(),
    )
    return jax.shard_map(
        per_device,
        mesh=mesh,
        in_specs=placed,
        out_specs=(
            P(None, "gx", "gy", None),
            P(None, "gx", "gy", None),
            P(None, None, "gx", "gy"),
            P(None, None, "gx", "gy"),
            P(None, None, None, "gx", "gy"),
        ),
        check_vma=False,
    )
```

```python
import math

import jax
import jax.numpy as jnp
import numpy as np
from jax import lax
from jax.experimental import pallas as pl
from jax.experimental.pallas import tpu as pltpu
from jax.sharding import PartitionSpec as P

WAVES = 256
TOP_PLANE = 111
BOTH = ("gx", "gy")
LANES = 128
SUBLANES = 8

curl_step = 0.5


def passed_along(value, axis, by):
    devices = lax.axis_size(axis)
    pairs = [(i, i + by) for i in range(devices) if 0 <= i + by < devices]
    return lax.ppermute(value, axis, pairs)


def passed_across(value, by_x, by_y):
    along_x, along_y = lax.axis_size("gx"), lax.axis_size("gy")
    pairs = [
        (x * along_y + y, (x + by_x) * along_y + y + by_y)
        for x in range(along_x)
        for y in range(along_y)
        if 0 <= x + by_x < along_x and 0 <= y + by_y < along_y
    ]
    return lax.ppermute(value, BOTH, pairs)


def swapped(value, by):
    devices = lax.axis_size(BOTH)
    return lax.ppermute(value, BOTH, [(i, i ^ by) for i in range(devices)])


def wave_tables(number, extent):
    wave = 2 * np.arange(number) + 1 - number
    angles = (wave[:, None] * np.arange(extent)[None, :] % (4 * number)) * (math.pi / (2 * number))
    return np.cos(angles), np.sin(angles)


def in_two(table):
    high = table.astype(np.float32).astype(jnp.bfloat16)
    low = (table - high.astype(np.float64)).astype(np.float32).astype(jnp.bfloat16)
    return jnp.asarray(high), jnp.asarray(low)


def forward_diff(values, along):
    padded = jnp.pad(values, [(0, 1) if which == along else (0, 0) for which in range(values.ndim)])
    return lax.slice_in_dim(padded, 1, values.shape[along] + 1, axis=along) - values


def backward_diff(values, along):
    padded = jnp.pad(values, [(1, 0) if which == along else (0, 0) for which in range(values.ndim)])
    return values - lax.slice_in_dim(padded, 0, values.shape[along], axis=along)


def ahead_diff(values, border, along):
    upper = lax.slice_in_dim(values, 1, values.shape[along], axis=along)
    return jnp.concatenate([upper, border], axis=along) - values


def behind_diff(values, border, along):
    lower = lax.slice_in_dim(values, 0, values.shape[along] - 1, axis=along)
    return values - jnp.concatenate([border, lower], axis=along)


def far_of(next_real, next_imag):
    highest = lax.Precision.HIGHEST
    comps, freqs, rows, cols = next_real.shape
    along_x, along_y = lax.axis_size("gx"), lax.axis_size("gy")
    devices = along_x * along_y
    planes = comps * freqs
    share = devices // planes
    part_rows = rows // share
    wide = WAVES // along_y
    part_wide = wide // share
    tall = WAVES // along_x
    place = lax.axis_index(BOTH) % share

    both = jnp.stack([next_real, next_imag]).reshape(2, planes, share, part_rows, cols)
    both = both.transpose(1, 2, 0, 3, 4).reshape(devices, 2, part_rows, cols)
    got = lax.all_to_all(both, BOTH, split_axis=0, concat_axis=0, tiled=True)
    got = got.reshape(along_x, along_y, 2, part_rows, cols)

    cos_y, sin_y = (table.astype(np.float32) for table in wave_tables(WAVES, cols * along_y))
    order_k = np.arange(WAVES).reshape(along_y, share, part_wide).transpose(1, 0, 2).reshape(-1)
    cos_y = cos_y[order_k].reshape(share, -1, along_y, cols)
    sin_y = sin_y[order_k].reshape(share, -1, along_y, cols)
    with_cos = jnp.einsum("gbirc,skbc->sigrk", got, cos_y, precision=highest)
    with_sin = jnp.einsum("gbirc,skbc->sigrk", got, sin_y, precision=highest)
    partial = jnp.stack([with_cos[:, 0] + with_sin[:, 1], with_cos[:, 1] - with_sin[:, 0]], axis=1)

    pieces = []
    for by in range(share):
        piece = lax.dynamic_index_in_dim(partial, place ^ by, 0, keepdims=False)
        pieces.append(piece if by == 0 else swapped(piece, by))
    pieces = jnp.stack(pieces)
    partial = jnp.stack(
        [lax.dynamic_index_in_dim(pieces, place ^ s, 0, keepdims=False) for s in range(share)]
    )

    cos_x, sin_x = (table.astype(np.float32) for table in wave_tables(WAVES, rows * along_x))
    cos_x = cos_x.reshape(WAVES, along_x, share, part_rows)
    sin_x = sin_x.reshape(WAVES, along_x, share, part_rows)
    with_cos = jnp.einsum("jgsr,sigrk->ijk", cos_x, partial, precision=highest)
    with_sin = jnp.einsum("jgsr,sigrk->ijk", sin_x, partial, precision=highest)
    far = jnp.stack([with_cos[0] + with_sin[1], with_cos[1] - with_sin[0]])
    far = far * (1.0 / math.sqrt(rows * along_x * cols * along_y))

    far = far.reshape(2, along_x, tall, along_y, part_wide).transpose(1, 3, 0, 2, 4)
    far = far.reshape(devices, 2, tall, part_wide)
    far = lax.all_to_all(far, BOTH, split_axis=0, concat_axis=0, tiled=True)
    far = far.reshape(comps, freqs, share, 2, tall, part_wide).transpose(3, 0, 1, 4, 2, 5)
    return far.reshape(2, comps, freqs, tall, wide)


def general_step(electric, magnetic, retention, coupling, spectrum_real, spectrum_imag, phases):
    elec_x, elec_y, elec_z = (electric[0], electric[1], electric[2])
    rows_elec = passed_along(electric[1:3, 0:1], "gx", -1)
    cols_elec = passed_along(electric[0:3:2, :, 0:1], "gy", -1)
    mag_x = magnetic[0] - curl_step * (
        ahead_diff(elec_z, cols_elec[1], 1) - forward_diff(elec_y, 2)
    )
    mag_y = magnetic[1] - curl_step * (
        forward_diff(elec_x, 2) - ahead_diff(elec_z, rows_elec[1], 0)
    )
    mag_z = magnetic[2] - curl_step * (
        ahead_diff(elec_y, rows_elec[0], 0) - ahead_diff(elec_x, cols_elec[0], 1)
    )
    next_magnetic = jnp.stack([mag_x, mag_y, mag_z])
    rows_magn = passed_along(next_magnetic[1:3, -1:], "gx", 1)
    cols_magn = passed_along(next_magnetic[0:3:2, :, -1:], "gy", 1)
    new_x = retention * elec_x + coupling * (
        behind_diff(mag_z, cols_magn[1], 1) - backward_diff(mag_y, 2)
    )
    new_y = retention * elec_y + coupling * (
        backward_diff(mag_x, 2) - behind_diff(mag_z, rows_magn[1], 0)
    )
    new_z = retention * elec_z + coupling * (
        behind_diff(mag_y, rows_magn[0], 0) - behind_diff(mag_x, cols_magn[0], 1)
    )
    next_electric = jnp.stack([new_x, new_y, new_z])
    tangent = jnp.stack(
        [
            new_x[:, :, TOP_PLANE],
            new_y[:, :, TOP_PLANE],
            mag_x[:, :, TOP_PLANE],
            mag_y[:, :, TOP_PLANE],
        ]
    )
    next_real = spectrum_real + tangent[:, None] * jnp.cos(phases)[None, :, None, None]
    next_imag = spectrum_imag - tangent[:, None] * jnp.sin(phases)[None, :, None, None]
    return (next_electric, next_magnetic, next_real, next_imag, far_of(next_real, next_imag))


def spot(shape, axis):
    return lax.broadcasted_iota(jnp.int32, shape, axis)


def moved(value, by, axis):
    by = by % value.shape[axis]
    return value if by == 0 else pltpu.roll(value, by, axis)


def after(value, axis, border=0.0):
    size = value.shape[axis]
    return jnp.where(spot(value.shape, axis) == size - 1, border, moved(value, -1, axis))


def before(value, axis, border=0.0):
    return jnp.where(spot(value.shape, axis) == 0, border, moved(value, 1, axis))


def whole_vmem():
    return pl.BlockSpec(memory_space=pltpu.VMEM)


def whole_smem():
    return pl.BlockSpec(memory_space=pltpu.SMEM)


PICKED = ((0, -1, 3), (1, -1, 3), (2, -1, 2), (3, -1, 2), (4, -1, 2), (5, 0, 1), (6, 0, 1), (7, 0, 1))


def spread_kernel(
    edge, cosine, sine, elec, magn, ret, coup, real, imag,
    out, rows_elec, rows_magn, cols_elec, cols_magn, corner_up, corner_down, planes, edges,
):
    step = pl.program_id(0)
    steps = pl.num_programs(0)
    deep = elec.shape[1]
    rows = planes.shape[0]
    lane = spot((LANES, LANES), 1)
    for at in range(deep):
        arrays = [elec[0, at], elec[1, at], elec[2, at], magn[0, at], magn[1, at], magn[2, at], ret[at], coup[at]]
        packed = None
        start = 0
        for which, first, count in PICKED:
            turned = moved(arrays[which], start - TOP_PLANE - first, 1)
            packed = turned if packed is None else jnp.where(lane < start, packed, turned)
            start += count
        planes[step * deep + at] = packed.T[0:16]
        edges[0, pl.ds(step * deep + at, 1), :] = elec[0, at, -1:, :]
        edges[1, pl.ds(step * deep + at, 1), :] = elec[1, at, -1:, :]
        edges[2, pl.ds(step * deep + at, 1), :] = magn[2, at, -1:, :]
        cols_elec[0, pl.ds(step * deep + at, 1), :] = elec[0, at, 0:1, :]
        cols_elec[1, pl.ds(step * deep + at, 1), :] = elec[2, at, 0:1, :]
        line = elec[1, at, -1:, :]
        cols_magn[0, pl.ds(step * deep + at, 1), :] = (
            magn[0, at, -1:, :] + curl_step * elec[2, at, -1:, :] + curl_step * (after(line, 1) - line)
        )

    @pl.when(step == 0)
    def _():
        rows_elec[0] = elec[1, 0]
        rows_elec[1] = elec[2, 0]
        corner_up[...] = jnp.broadcast_to(elec[1, 0, -1:, :], corner_up.shape)

    @pl.when(step == steps - 1)
    def _():
        last = deep - 1
        ex, ey, ez = elec[0, last], elec[1, last], elec[2, last]
        rows_magn[0] = magn[1, last] - curl_step * (after(ex, 1) - ex) - curl_step * ez
        rows_magn[1] = magn[2, last] + curl_step * ey + curl_step * (after(ex, 0) - ex)
        corner_down[...] = jnp.broadcast_to(elec[0, last, 0:1, :], corner_down.shape)
        end_x, end_y, end_z = edges[0], edges[1], edges[2]
        cols_magn[1] = end_z - curl_step * (after(end_y, 0) - end_y) - curl_step * end_x

        ex_m, ex_p, ex_q, ey_m, ey_p, ey_q, ez_m, ez_p, hx_m, hx_p, hy_m, hy_p, hz_p, keep, gain = (
            planes[:, which, :] for which in range(15)
        )
        hx_p = hx_p - curl_step * ((after(ez_p, 1) - ez_p) - (ey_q - ey_p))
        hx_m = hx_m - curl_step * ((after(ez_m, 1) - ez_m) - (ey_p - ey_m))
        hy_p = hy_p - curl_step * ((ex_q - ex_p) - (after(ez_p, 0) - ez_p))
        hy_m = hy_m - curl_step * ((ex_p - ex_m) - (after(ez_m, 0) - ez_m))
        hz_p = hz_p - curl_step * ((after(ey_p, 0) - ey_p) - (after(ex_p, 1) - ex_p))
        edge_x, edge_y = curl_step * edge[0], curl_step * edge[1]
        tangent = (
            keep * ex_p + gain * ((hz_p - before(hz_p, 1, edge_y * ex_p)) - (hy_p - hy_m)),
            keep * ey_p + gain * ((hx_p - hx_m) - (hz_p - before(hz_p, 0, -edge_x * ey_p))),
            hx_p,
            hy_p,
        )
        ez_jump = curl_step * (ez_p - ez_m)
        push = -curl_step * ey_p
        none = jnp.zeros_like(ex_p)
        one = jnp.ones_like(ex_p)
        row_up = (push - before(push, 1) - ez_jump, -push, none, curl_step * ez_p)
        row_down = (none, hz_p, none, none)
        col_left = (
            curl_step * ex_p,
            -ez_jump - curl_step * ex_p + before(curl_step * ex_p, 0),
            -curl_step * ez_p,
            none,
        )
        col_right = (-hz_p, none, none, none)
        wide = lax.broadcasted_iota(jnp.int32, (LANES, LANES), 1)
        tall = lax.broadcasted_iota(jnp.int32, (SUBLANES, LANES), 0)
        lanes = lax.broadcasted_iota(jnp.int32, (SUBLANES, LANES), 1)
        pad = jnp.zeros((LANES - rows, LANES), jnp.float32)

        def upright(lines):
            block = None
            for which, (value, column) in enumerate(lines):
                value = moved(value, which - column, 1)
                block = value if block is None else jnp.where(wide[0:rows] < which, block, value)
            return jnp.concatenate([block, pad], axis=0).T[0:SUBLANES]

        end = LANES - 1
        for comp in range(4):
            factor = gain if comp < 2 else one
            upright_lines = upright(
                [(none, 0), (none, 0), (none, 0), (none, 0), (col_left[comp], 0), (col_right[comp], end), (factor, end), (factor, 0)]
            )
            extra = jnp.where(tall >= 4, upright_lines, 0.0)
            extra = jnp.where(tall == 0, row_up[comp][0:1], extra)
            extra = jnp.where(tall == 1, row_down[comp][rows - 1 :], extra)
            extra = jnp.where(tall == 2, factor[rows - 1 :], extra)
            extra = jnp.where(tall == 3, factor[0:1], extra)
            if comp == 0:
                spare = moved(-push[0:1], rows - end, 1)
                extra = jnp.where((tall == 5) & (lanes == rows), spare, extra)
            if comp == 1:
                spare = moved(curl_step * ex_p[rows - 1 :], rows, 1)
                extra = jnp.where((tall == 4) & (lanes == rows), spare, extra)
            freqs = real.shape[1]
            for freq in range(freqs):
                new_real = real[comp, freq] + tangent[comp] * cosine[freq]
                new_imag = imag[comp, freq] - tangent[comp] * sine[freq]
                for half in range(2):
                    to = (comp * freqs + freq) * 2 + half
                    out[to, 0:8] = new_real[half * 8 : half * 8 + 8]
                    out[to, 8:16] = new_imag[half * 8 : half * 8 + 8]
                    out[to, 16:24] = extra


def spread(edge, electric, magnetic, retention, coupling, spectrum_real, spectrum_imag, cosine, sine):
    _, rows, cols, deep = electric.shape
    comps, freqs = spectrum_real.shape[:2]
    slab = 4
    vector = pl.BlockSpec((3, slab, cols, deep), lambda i: (0, i, 0, 0))
    scalar = pl.BlockSpec((slab, cols, deep), lambda i: (i, 0, 0))
    kind = jnp.float32
    return pl.pallas_call(
        spread_kernel,
        grid=(rows // slab,),
        in_specs=[whole_smem(), whole_smem(), whole_smem(), vector, vector, scalar, scalar, whole_vmem(), whole_vmem()],
        out_specs=[whole_vmem()] * 7,
        out_shape=[
            jax.ShapeDtypeStruct((comps * freqs * 2, 24, cols), kind),
            jax.ShapeDtypeStruct((2, cols, deep), kind),
            jax.ShapeDtypeStruct((2, cols, deep), kind),
            jax.ShapeDtypeStruct((2, rows, deep), kind),
            jax.ShapeDtypeStruct((2, rows, deep), kind),
            jax.ShapeDtypeStruct((SUBLANES, deep), kind),
            jax.ShapeDtypeStruct((SUBLANES, deep), kind),
        ],
        scratch_shapes=[pltpu.VMEM((rows, 16, LANES), kind), pltpu.VMEM((3, rows, LANES), kind)],
        name="spread",
    )(edge, cosine, sine, electric, magnetic, retention, coupling, spectrum_real, spectrum_imag)


def split_high(value):
    high = value.astype(jnp.bfloat16)
    return high, (value - high.astype(jnp.float32)).astype(jnp.bfloat16)


def dot(a, b):
    return jnp.dot(a, b, preferred_element_type=jnp.float32)


def along_y_kernel(at, cosine, sine, got, high, low, mine, other, lines):
    along_x, along_y = got.shape[0], got.shape[1]
    blocks = along_x * along_y
    half = at[0] % 2
    freq = (at[0] // 2) % cosine.shape[0]
    weight_real = cosine[freq]
    weight_imag = -sine[freq]
    is_last = jnp.where(half == 1, 1.0, 0.0)
    is_first = jnp.where(half == 0, 1.0, 0.0)

    def column(which):
        return jnp.concatenate([got[x, :, 16 + which, :] for x in range(along_x)], axis=0)

    block = spot((blocks, LANES), 0)
    lane = spot((blocks, LANES), 1)
    inner = block % along_y
    rows = 16
    from_right = jnp.where(inner == along_y - 1, 0.0, moved(column(4), -1, 0))
    from_left = jnp.where(inner == 0, 0.0, moved(column(5), 1, 0))
    right_up = jnp.where(block < along_y, 0.0, moved(from_right, along_y, 0))
    left_down = jnp.where(block >= blocks - along_y, 0.0, moved(from_left, -along_y, 0))
    from_right = from_right + jnp.where(lane == 0, moved(right_up, -rows, 1), 0.0)
    from_left = from_left + jnp.where(lane == rows - 1, moved(left_down, -1, 1), 0.0)
    last_col = column(6) * from_right
    first_col = column(7) * from_left
    pad = jnp.zeros((LANES - 2 * blocks, LANES), jnp.float32)
    upright = jnp.concatenate([last_col, first_col, pad], axis=0).T
    cols = jnp.where(half == 0, upright[0:8], upright[8:16])

    low_row = spot((SUBLANES, LANES), 0)
    low_lane = spot((SUBLANES, LANES), 1)
    for x in range(along_x):
        for y in range(along_y):
            here = x * along_y + y
            delta = jnp.where(low_lane == LANES - 1, moved(cols, LANES - 1 - here, 1), 0.0)
            delta = delta + jnp.where(low_lane == 0, moved(cols, -blocks - here, 1), 0.0)
            if x + 1 < along_x:
                row = got[x, y, 18:19, :] * got[x + 1, y, 16:17, :] * is_last
                delta = delta + jnp.where(low_row == SUBLANES - 1, row, 0.0)
            if x > 0:
                row = got[x, y, 19:20, :] * got[x - 1, y, 17:18, :] * is_first
                delta = delta + jnp.where(low_row == 0, row, 0.0)
            span = slice(y * LANES, (y + 1) * LANES)
            lines[x * 16 : x * 16 + 8, span] = got[x, y, 0:8, :] + weight_real * delta
            lines[x * 16 + 8 : x * 16 + 16, span] = got[x, y, 8:16, :] + weight_imag * delta

    lines_high, lines_low = split_high(lines[...])
    total = dot(lines_high, high[...]) + (dot(lines_low, high[...]) + dot(lines_high, low[...]))
    waves = total.shape[1] // 2
    piece = waves // 2
    for x in range(along_x):
        top = total[x * 16 : x * 16 + 8]
        bottom = total[x * 16 + 8 : x * 16 + 16]
        new_real = top[:, :waves] + bottom[:, waves:]
        new_imag = bottom[:, :waves] - top[:, waves:]
        span = slice(x * 8, x * 8 + 8)
        mine[span, :piece] = jnp.where(half == 0, new_real[:, :piece], new_real[:, piece:])
        mine[span, piece:] = jnp.where(half == 0, new_imag[:, :piece], new_imag[:, piece:])
        other[span, :piece] = jnp.where(half == 0, new_real[:, piece:], new_real[:, :piece])
        other[span, piece:] = jnp.where(half == 0, new_imag[:, piece:], new_imag[:, :piece])


def along_y_sums(place, cosine, sine, got, cols, along_x, along_y):
    wide = WAVES // along_y
    order = np.arange(WAVES).reshape(along_y, 2, wide // 2).transpose(1, 0, 2).reshape(-1)
    cos_y, sin_y = wave_tables(WAVES, cols * along_y)
    high, low = in_two(np.concatenate([cos_y[order].T, sin_y[order].T], axis=1))
    shape = jax.ShapeDtypeStruct((along_x * 8, WAVES), jnp.float32)
    return pl.pallas_call(
        along_y_kernel,
        in_specs=[whole_smem()] * 3 + [whole_vmem()] * 3,
        out_specs=[whole_vmem()] * 2,
        out_shape=[shape, shape],
        scratch_shapes=[pltpu.VMEM((along_x * 16, along_y * LANES), jnp.float32)],
        name="along_y",
    )(place, cosine, sine, got.reshape(along_x, along_y, 24, cols), high, low)


def along_x_kernel(along_x, at, mine, other, high, low, out):
    half = at[0] % 2
    lines = jnp.concatenate(
        [jnp.where(half == 0, mine[...], other[...]), jnp.where(half == 0, other[...], mine[...])], axis=0
    )
    lines_high, lines_low = split_high(lines)
    total = dot(high[...], lines_high) + (dot(high[...], lines_low) + dot(low[...], lines_high))
    waves = total.shape[0] // 2
    piece = total.shape[1] // 2
    far = (
        total[:waves, :piece] + total[waves:, piece:],
        total[:waves, piece:] - total[waves:, :piece],
    )
    tall = waves // along_x
    stacks = tall // SUBLANES
    along_y = out.shape[0] // along_x
    wide = piece // along_y
    lane = spot((SUBLANES, LANES), 1)
    for x in range(along_x):
        for part in range(2):
            tiles = [far[part][x * tall + q * 8 : x * tall + q * 8 + 8] for q in range(stacks)]
            for y in range(along_y):
                block = None
                for q in range(stacks):
                    tile = moved(tiles[q], (q - y) * wide, 1)
                    block = tile if block is None else jnp.where(lane < q * wide, block, tile)
                out[x * along_y + y, part * 8 : part * 8 + 8] = block


def along_x_sums(place, mine, other, rows, scale, along_x, devices):
    cos_x, sin_x = wave_tables(WAVES, rows * along_x)
    table = np.concatenate([cos_x, sin_x], axis=0) * scale
    table = table.reshape(2 * WAVES, along_x, 2, 8).transpose(0, 2, 1, 3).reshape(2 * WAVES, rows * along_x)
    high, low = in_two(table)
    return pl.pallas_call(
        lambda *refs: along_x_kernel(along_x, *refs),
        in_specs=[whole_smem()] + [whole_vmem()] * 4,
        out_specs=whole_vmem(),
        out_shape=jax.ShapeDtypeStruct((devices, 16, LANES), jnp.float32),
        name="along_x",
    )(place, mine, other, high, low)


def placed_kernel(got, out):
    planes, tall, wide = out.shape[1:]
    piece = wide // 2
    lane = spot((SUBLANES, LANES), 1)
    for plane in range(planes):
        for part in range(2):
            first = got[2 * plane, part * 8 : part * 8 + 8]
            second = got[2 * plane + 1, part * 8 : part * 8 + 8]
            for q in range(tall // SUBLANES):
                tile = jnp.where(lane < piece, moved(first, -q * piece, 1), moved(second, piece - q * piece, 1))
                out[part, plane, q * 8 : q * 8 + 8, :] = tile[:, :wide]


def placed_far(got, comps, freqs, tall, wide):
    far = pl.pallas_call(
        placed_kernel,
        in_specs=[whole_vmem()],
        out_specs=whole_vmem(),
        out_shape=jax.ShapeDtypeStruct((2, comps * freqs, tall, wide), jnp.float32),
        name="placed",
    )(got)
    return far.reshape(2, comps, freqs, tall, wide)


def yee_kernel(
    edge, cosine, sine, elec, ahead, magn, ret, coup, rows_elec, rows_magn, cols_elec, cols_magn, corner_up, corner_down,
    real, imag, new_elec, new_magn, new_real, new_imag, carried, tops,
):
    step = pl.program_id(0)
    steps = pl.num_programs(0)
    deep = elec.shape[1]
    inner_x = edge[0]
    inner_y = edge[1]
    row = spot((LANES, LANES), 0)
    lane = spot((LANES, LANES), 1)

    @pl.when(step == 0)
    def _():
        spare = jnp.where(row == LANES - 1, curl_step * corner_down[0:1, :], 0.0)
        carried[0] = (rows_magn[0] + curl_step * elec[2, 0]) * inner_x
        carried[1] = (rows_magn[1] - curl_step * elec[1, 0] + spare) * inner_x

    at_end = step == steps - 1
    for at in range(deep):
        here = pl.ds(step * deep + at, 1)
        ex, ey, ez = elec[0, at], elec[1, at], elec[2, at]
        if at + 1 < deep:
            ey_next, ez_next = elec[1, at + 1], elec[2, at + 1]
        else:
            ey_next = jnp.where(at_end, rows_elec[0], ahead[1, 0])
            ez_next = jnp.where(at_end, rows_elec[1], ahead[2, 0])
        hx = magn[0, at] - curl_step * ((after(ez, 0, cols_elec[1, here, :]) - ez) - (after(ey, 1) - ey))
        hy = magn[1, at] - curl_step * ((after(ex, 1) - ex) - (ez_next - ez))
        hz = magn[2, at] - curl_step * ((ey_next - ey) - (after(ex, 0, cols_elec[0, here, :]) - ex))
        new_magn[0, at] = hx
        new_magn[1, at] = hy
        new_magn[2, at] = hz
        side_x = (cols_magn[0, here, :] - curl_step * ez[0:1]) * inner_y
        side_z = cols_magn[1, here, :] + curl_step * ex[0:1]
        if at + 1 == deep:
            side_z = side_z - jnp.where(at_end, curl_step * corner_up[0:1, :], 0.0)
        side_z = side_z * inner_y
        keep, gain = ret[at], coup[at]
        new_x = keep * ex + gain * ((hz - before(hz, 0, side_z)) - (hy - before(hy, 1)))
        new_y = keep * ey + gain * ((hx - before(hx, 1)) - (hz - carried[1]))
        new_z = keep * ez + gain * ((hy - carried[0]) - (hx - before(hx, 0, side_x)))
        new_elec[0, at] = new_x
        new_elec[1, at] = new_y
        new_elec[2, at] = new_z
        carried[0] = hy
        carried[1] = hz
        packed = None
        for which, value in enumerate((new_x, new_y, hx, hy)):
            turned = moved(value, which - TOP_PLANE, 1)
            packed = turned if packed is None else jnp.where(lane < which, packed, turned)
        tops[step * deep + at] = packed.T[0:SUBLANES]

    @pl.when(at_end)
    def _():
        for comp in range(4):
            tangent = tops[:, comp, :]
            for freq in range(real.shape[1]):
                new_real[comp, freq] = real[comp, freq] + tangent * cosine[freq]
                new_imag[comp, freq] = imag[comp, freq] - tangent * sine[freq]


def yee(edge, cosine, sine, electric, magnetic, retention, coupling, halos, spectrum_real, spectrum_imag):
    _, rows, cols, deep = electric.shape
    slab = 2
    steps = rows // slab
    vector = pl.BlockSpec((3, slab, cols, deep), lambda i: (0, i, 0, 0))
    ahead = pl.BlockSpec((3, 1, cols, deep), lambda i: (0, jnp.minimum((i + 1) * slab, rows - 1), 0, 0))
    scalar = pl.BlockSpec((slab, cols, deep), lambda i: (i, 0, 0))
    kind = jnp.float32
    return pl.pallas_call(
        yee_kernel,
        grid=(steps,),
        in_specs=[whole_smem()] * 3 + [vector, ahead, vector, scalar, scalar] + [whole_vmem()] * 8,
        out_specs=[vector, vector, whole_vmem(), whole_vmem()],
        out_shape=[
            jax.ShapeDtypeStruct(electric.shape, kind),
            jax.ShapeDtypeStruct(magnetic.shape, kind),
            jax.ShapeDtypeStruct(spectrum_real.shape, kind),
            jax.ShapeDtypeStruct(spectrum_imag.shape, kind),
        ],
        scratch_shapes=[pltpu.VMEM((2, cols, deep), kind), pltpu.VMEM((rows, SUBLANES, LANES), kind)],
        cost_estimate=pl.CostEstimate(flops=60 * electric.size, bytes_accessed=20 * electric.size, transcendentals=0),
        name="yee",
    )(edge, cosine, sine, electric, electric, magnetic, retention, coupling, *halos, spectrum_real, spectrum_imag)


def tiled_step(electric, magnetic, retention, coupling, spectrum_real, spectrum_imag, phases):
    comps, freqs, rows, cols = spectrum_real.shape
    along_x, along_y = lax.axis_size("gx"), lax.axis_size("gy")
    devices = along_x * along_y
    cosine, sine = jnp.cos(phases), jnp.sin(phases)
    place = lax.axis_index(BOTH).astype(jnp.int32).reshape(1)
    edge = jnp.stack([lax.axis_index("gx") > 0, lax.axis_index("gy") > 0]).astype(jnp.float32)
    sent, rows_elec, rows_magn, cols_elec, cols_magn, corner_up, corner_down = spread(
        edge, electric, magnetic, retention, coupling, spectrum_real, spectrum_imag, cosine, sine
    )
    got = lax.all_to_all(sent, BOTH, split_axis=0, concat_axis=0, tiled=True)
    halos = (
        passed_along(rows_elec, "gx", -1),
        passed_along(rows_magn, "gx", 1),
        passed_along(cols_elec, "gy", -1),
        passed_along(cols_magn, "gy", 1),
        passed_across(corner_up, -1, 1),
        passed_across(corner_down, 1, -1),
    )
    mine, other = along_y_sums(place, cosine, sine, got, cols, along_x, along_y)
    other = swapped(other, 1)
    scale = 1.0 / math.sqrt(rows * along_x * cols * along_y)
    far = along_x_sums(place, mine, other, rows, scale, along_x, devices)
    far = lax.all_to_all(far, BOTH, split_axis=0, concat_axis=0, tiled=True)
    next_electric, next_magnetic, next_real, next_imag = yee(
        edge, cosine, sine, electric, magnetic, retention, coupling, halos, spectrum_real, spectrum_imag
    )
    far_field = placed_far(far, comps, freqs, WAVES // along_x, WAVES // along_y)
    return (next_electric, next_magnetic, next_real, next_imag, far_field)


def per_device(*arrays):
    comps, freqs, rows, cols = arrays[4].shape
    depth = arrays[0].shape[3]
    along_x, along_y = lax.axis_size("gx"), lax.axis_size("gy")
    wide, tall = WAVES // along_y, WAVES // along_x
    fits = (
        comps == 4
        and along_x * along_y == 2 * comps * freqs
        and (rows, cols, depth) == (2 * SUBLANES, LANES, LANES)
        and WAVES == 2 * LANES
        and (wide // 2) * (tall // SUBLANES) == LANES
        and 0 < TOP_PLANE < depth - 1
    )
    return tiled_step(*arrays) if fits else general_step(*arrays)


def solution(mesh):
    placed = (
        P(None, "gx", "gy", None),
        P(None, "gx", "gy", None),
        P("gx", "gy", None),
        P("gx", "gy", None),
        P(None, None, "gx", "gy"),
        P(None, None, "gx", "gy"),
        P(),
    )
    return jax.shard_map(
        per_device,
        mesh=mesh,
        in_specs=placed,
        out_specs=(
            P(None, "gx", "gy", None),
            P(None, "gx", "gy", None),
            P(None, None, "gx", "gy"),
            P(None, None, "gx", "gy"),
            P(None, None, None, "gx", "gy"),
        ),
        check_vma=False,
    )
```

```python
import math

import jax
import jax.numpy as jnp
import numpy as np
from jax import lax
from jax.experimental import pallas as pl
from jax.experimental.pallas import tpu as pltpu
from jax.sharding import PartitionSpec as P


WAVES = 256
TOP_PLANE = 111
BOTH = ("gx", "gy")
LANES = 128
SUBLANES = 8

curl_step = 0.5


def passed_along(value, axis, by):
    devices = lax.axis_size(axis)
    pairs = [(i, i + by) for i in range(devices) if 0 <= i + by < devices]
    return lax.ppermute(value, axis, pairs)


def swapped(value, by):
    devices = lax.axis_size(BOTH)
    return lax.ppermute(value, BOTH, [(i, i ^ by) for i in range(devices)])


def wave_tables(number, extent):
    wave = 2 * np.arange(number) + 1 - number
    angles = (wave[:, None] * np.arange(extent)[None, :] % (4 * number)) * (math.pi / (2 * number))
    return np.cos(angles), np.sin(angles)


def in_two(table):
    high = table.astype(np.float32).astype(jnp.bfloat16)
    low = (table - high.astype(np.float64)).astype(np.float32).astype(jnp.bfloat16)
    return jnp.asarray(high), jnp.asarray(low)


def forward_diff(values, along):
    padded = jnp.pad(values, [(0, 1) if which == along else (0, 0) for which in range(values.ndim)])
    return lax.slice_in_dim(padded, 1, values.shape[along] + 1, axis=along) - values


def backward_diff(values, along):
    padded = jnp.pad(values, [(1, 0) if which == along else (0, 0) for which in range(values.ndim)])
    return values - lax.slice_in_dim(padded, 0, values.shape[along], axis=along)


def ahead_diff(values, border, along):
    upper = lax.slice_in_dim(values, 1, values.shape[along], axis=along)
    return jnp.concatenate([upper, border], axis=along) - values


def behind_diff(values, border, along):
    lower = lax.slice_in_dim(values, 0, values.shape[along] - 1, axis=along)
    return values - jnp.concatenate([border, lower], axis=along)


def far_of(next_real, next_imag):
    highest = lax.Precision.HIGHEST
    comps, freqs, rows, cols = next_real.shape
    along_x, along_y = lax.axis_size("gx"), lax.axis_size("gy")
    devices = along_x * along_y
    planes = comps * freqs
    share = devices // planes
    part_rows = rows // share
    wide = WAVES // along_y
    part_wide = wide // share
    tall = WAVES // along_x
    place = lax.axis_index(BOTH) % share

    both = jnp.stack([next_real, next_imag]).reshape(2, planes, share, part_rows, cols)
    both = both.transpose(1, 2, 0, 3, 4).reshape(devices, 2, part_rows, cols)
    got = lax.all_to_all(both, BOTH, split_axis=0, concat_axis=0, tiled=True)
    got = got.reshape(along_x, along_y, 2, part_rows, cols)

    cos_y, sin_y = (table.astype(np.float32) for table in wave_tables(WAVES, cols * along_y))
    order_k = np.arange(WAVES).reshape(along_y, share, part_wide).transpose(1, 0, 2).reshape(-1)
    cos_y = cos_y[order_k].reshape(share, -1, along_y, cols)
    sin_y = sin_y[order_k].reshape(share, -1, along_y, cols)
    with_cos = jnp.einsum("gbirc,skbc->sigrk", got, cos_y, precision=highest)
    with_sin = jnp.einsum("gbirc,skbc->sigrk", got, sin_y, precision=highest)
    partial = jnp.stack([with_cos[:, 0] + with_sin[:, 1], with_cos[:, 1] - with_sin[:, 0]], axis=1)

    pieces = []
    for by in range(share):
        piece = lax.dynamic_index_in_dim(partial, place ^ by, 0, keepdims=False)
        pieces.append(piece if by == 0 else swapped(piece, by))
    pieces = jnp.stack(pieces)
    partial = jnp.stack(
        [lax.dynamic_index_in_dim(pieces, place ^ s, 0, keepdims=False) for s in range(share)]
    )

    cos_x, sin_x = (table.astype(np.float32) for table in wave_tables(WAVES, rows * along_x))
    cos_x = cos_x.reshape(WAVES, along_x, share, part_rows)
    sin_x = sin_x.reshape(WAVES, along_x, share, part_rows)
    with_cos = jnp.einsum("jgsr,sigrk->ijk", cos_x, partial, precision=highest)
    with_sin = jnp.einsum("jgsr,sigrk->ijk", sin_x, partial, precision=highest)
    far = jnp.stack([with_cos[0] + with_sin[1], with_cos[1] - with_sin[0]])
    far = far * (1.0 / math.sqrt(rows * along_x * cols * along_y))

    far = far.reshape(2, along_x, tall, along_y, part_wide).transpose(1, 3, 0, 2, 4)
    far = far.reshape(devices, 2, tall, part_wide)
    far = lax.all_to_all(far, BOTH, split_axis=0, concat_axis=0, tiled=True)
    far = far.reshape(comps, freqs, share, 2, tall, part_wide).transpose(3, 0, 1, 4, 2, 5)
    return far.reshape(2, comps, freqs, tall, wide)


def general_step(electric, magnetic, retention, coupling, spectrum_real, spectrum_imag, phases):
    elec_x, elec_y, elec_z = (electric[0], electric[1], electric[2])
    rows_elec = passed_along(electric[1:3, 0:1], "gx", -1)
    cols_elec = passed_along(electric[0:3:2, :, 0:1], "gy", -1)
    mag_x = magnetic[0] - curl_step * (
        ahead_diff(elec_z, cols_elec[1], 1) - forward_diff(elec_y, 2)
    )
    mag_y = magnetic[1] - curl_step * (
        forward_diff(elec_x, 2) - ahead_diff(elec_z, rows_elec[1], 0)
    )
    mag_z = magnetic[2] - curl_step * (
        ahead_diff(elec_y, rows_elec[0], 0) - ahead_diff(elec_x, cols_elec[0], 1)
    )
    next_magnetic = jnp.stack([mag_x, mag_y, mag_z])
    rows_magn = passed_along(next_magnetic[1:3, -1:], "gx", 1)
    cols_magn = passed_along(next_magnetic[0:3:2, :, -1:], "gy", 1)
    new_x = retention * elec_x + coupling * (
        behind_diff(mag_z, cols_magn[1], 1) - backward_diff(mag_y, 2)
    )
    new_y = retention * elec_y + coupling * (
        backward_diff(mag_x, 2) - behind_diff(mag_z, rows_magn[1], 0)
    )
    new_z = retention * elec_z + coupling * (
        behind_diff(mag_y, rows_magn[0], 0) - behind_diff(mag_x, cols_magn[0], 1)
    )
    next_electric = jnp.stack([new_x, new_y, new_z])
    tangent = jnp.stack(
        [
            new_x[:, :, TOP_PLANE],
            new_y[:, :, TOP_PLANE],
            mag_x[:, :, TOP_PLANE],
            mag_y[:, :, TOP_PLANE],
        ]
    )
    next_real = spectrum_real + tangent[:, None] * jnp.cos(phases)[None, :, None, None]
    next_imag = spectrum_imag - tangent[:, None] * jnp.sin(phases)[None, :, None, None]
    return (next_electric, next_magnetic, next_real, next_imag, far_of(next_real, next_imag))


def spot(shape, axis):
    return lax.broadcasted_iota(jnp.int32, shape, axis)


def moved(value, by, axis):
    by = by % value.shape[axis]
    return value if by == 0 else pltpu.roll(value, by, axis)


def after(value, axis, border=0.0):
    size = value.shape[axis]
    return jnp.where(spot(value.shape, axis) == size - 1, border, moved(value, -1, axis))


def before(value, axis, border=0.0):
    return jnp.where(spot(value.shape, axis) == 0, border, moved(value, 1, axis))


def whole_vmem():
    return pl.BlockSpec(memory_space=pltpu.VMEM)


def kept(value):
    return pltpu.with_memory_space_constraint(value, pltpu.VMEM)


def far_kept(value):
    return pltpu.with_memory_space_constraint(value, pltpu.HBM)


def room(shape, dtype=jnp.float32):
    return pltpu.VMEM(shape, dtype)


def limited(size=24):
    return pltpu.CompilerParams(vmem_limit_bytes=size * 1024 * 1024)


def whole_smem():
    return pl.BlockSpec(memory_space=pltpu.SMEM)


PICKED = ((0, -1, 3), (1, -1, 3), (2, -1, 2), (3, -1, 2), (4, -1, 2), (5, 0, 1), (6, 0, 1), (7, 0, 1))


def spread_kernel(
    edge, cosine, sine, elec, magn, ret, coup, real_far, imag_far,
    out, rows_elec, rows_magn, cols_elec, cols_magn, planes, edges, corners, real, imag, arrived,
):
    step = pl.program_id(0)
    steps = pl.num_programs(0)
    deep = elec.shape[1]
    rows = planes.shape[0]
    lane = spot((LANES, LANES), 1)
    for at in range(deep):
        arrays = [elec[0, at], elec[1, at], elec[2, at], magn[0, at], magn[1, at], magn[2, at], ret[at], coup[at]]
        packed = None
        start = 0
        for which, first, count in PICKED:
            turned = moved(arrays[which], start - TOP_PLANE - first, 1)
            packed = turned if packed is None else jnp.where(lane < start, packed, turned)
            start += count
        planes[step * deep + at] = packed.T[0:16]
        edges[0, pl.ds(step * deep + at, 1), :] = elec[0, at, -1:, :]
        edges[1, pl.ds(step * deep + at, 1), :] = elec[1, at, -1:, :]
        edges[2, pl.ds(step * deep + at, 1), :] = magn[2, at, -1:, :]
        cols_elec[0, pl.ds(step * deep + at, 1), :] = elec[0, at, 0:1, :]
        cols_elec[1, pl.ds(step * deep + at, 1), :] = elec[2, at, 0:1, :]
        line = elec[1, at, -1:, :]
        cols_magn[0, pl.ds(step * deep + at, 1), :] = (
            magn[0, at, -1:, :] + curl_step * elec[2, at, -1:, :] + curl_step * (after(line, 1) - line)
        )

    real_copy = pltpu.make_async_copy(real_far, real, arrived.at[0])
    imag_copy = pltpu.make_async_copy(imag_far, imag, arrived.at[1])

    @pl.when(step == 0)
    def _():
        real_copy.start()
        imag_copy.start()
        rows_elec[0] = elec[1, 0]
        rows_elec[1] = elec[2, 0]
        corners[0:1, :] = elec[1, 0, -1:, :]

    @pl.when(step == steps - 1)
    def _():
        last = deep - 1
        ex, ey, ez = elec[0, last], elec[1, last], elec[2, last]
        rows_magn[0] = magn[1, last] - curl_step * (after(ex, 1) - ex) - curl_step * ez
        rows_magn[1] = magn[2, last] + curl_step * ey + curl_step * (after(ex, 0) - ex)
        corners[1:2, :] = elec[0, last, 0:1, :]
        end_x, end_y, end_z = edges[0], edges[1], edges[2]
        cols_magn[1] = end_z - curl_step * (after(end_y, 0) - end_y) - curl_step * end_x

        ex_m, ex_p, ex_q, ey_m, ey_p, ey_q, ez_m, ez_p, hx_m, hx_p, hy_m, hy_p, hz_p, keep, gain = (
            planes[:, which, :] for which in range(15)
        )
        hx_p = hx_p - curl_step * ((after(ez_p, 1) - ez_p) - (ey_q - ey_p))
        hx_m = hx_m - curl_step * ((after(ez_m, 1) - ez_m) - (ey_p - ey_m))
        hy_p = hy_p - curl_step * ((ex_q - ex_p) - (after(ez_p, 0) - ez_p))
        hy_m = hy_m - curl_step * ((ex_p - ex_m) - (after(ez_m, 0) - ez_m))
        hz_p = hz_p - curl_step * ((after(ey_p, 0) - ey_p) - (after(ex_p, 1) - ex_p))
        edge_x, edge_y = curl_step * edge[0], curl_step * edge[1]
        tangent = (
            keep * ex_p + gain * ((hz_p - before(hz_p, 1, edge_y * ex_p)) - (hy_p - hy_m)),
            keep * ey_p + gain * ((hx_p - hx_m) - (hz_p - before(hz_p, 0, -edge_x * ey_p))),
            hx_p,
            hy_p,
        )
        ez_jump = curl_step * (ez_p - ez_m)
        push = -curl_step * ey_p
        none = jnp.zeros_like(ex_p)
        one = jnp.ones_like(ex_p)
        row_up = (push - before(push, 1) - ez_jump, -push, none, curl_step * ez_p)
        row_down = (none, hz_p, none, none)
        col_left = (
            curl_step * ex_p,
            -ez_jump - curl_step * ex_p + before(curl_step * ex_p, 0),
            -curl_step * ez_p,
            none,
        )
        col_right = (-hz_p, none, none, none)
        wide = lax.broadcasted_iota(jnp.int32, (LANES, LANES), 1)
        tall = lax.broadcasted_iota(jnp.int32, (SUBLANES, LANES), 0)
        lanes = lax.broadcasted_iota(jnp.int32, (SUBLANES, LANES), 1)
        pad = jnp.zeros((LANES - rows, LANES), jnp.float32)

        def upright(lines):
            block = None
            for which, (value, column) in enumerate(lines):
                value = moved(value, which - column, 1)
                block = value if block is None else jnp.where(wide[0:rows] < which, block, value)
            return jnp.concatenate([block, pad], axis=0).T[0:SUBLANES]

        end = LANES - 1
        real_copy.wait()
        imag_copy.wait()
        for comp in range(4):
            factor = gain if comp < 2 else one
            columns = upright([(col_left[comp], 0), (col_right[comp], end), (factor, end), (factor, 0)])
            columns = sum(moved(columns[which : which + 1], which * rows, 1) for which in range(4))
            if comp < 2:
                spare = moved(-push[0:1], -end, 1) if comp == 0 else curl_step * ex_p[rows - 1 :]
                columns = jnp.where(lanes[0:1] == 4 * rows, moved(spare, 4 * rows, 1), columns)
            extra = jnp.where(tall == 0, row_up[comp][0:1], 0.0)
            extra = jnp.where(tall == 1, row_down[comp][rows - 1 :], extra)
            extra = jnp.where(tall == 2, factor[rows - 1 :], extra)
            extra = jnp.where(tall == 3, factor[0:1], extra)
            extra = jnp.where(tall == 4, columns, extra)
            extra = jnp.where(tall == 5, corners[0:1, :], extra)
            extra = jnp.where(tall == 6, corners[1:2, :], extra)
            freqs = real.shape[1]
            for freq in range(freqs):
                new_real = real[comp, freq] + tangent[comp] * cosine[freq]
                new_imag = imag[comp, freq] - tangent[comp] * sine[freq]
                for half in range(2):
                    to = (comp * freqs + freq) * 2 + half
                    out[to, 0:8] = new_real[half * 8 : half * 8 + 8]
                    out[to, 8:16] = new_imag[half * 8 : half * 8 + 8]
                    out[to, 16:24] = extra


def spread(edge, electric, magnetic, retention, coupling, spectrum_real, spectrum_imag, cosine, sine):
    _, rows, cols, deep = electric.shape
    comps, freqs = spectrum_real.shape[:2]
    slab = 4
    vector = pl.BlockSpec((3, slab, cols, deep), lambda i: (0, i, 0, 0))
    scalar = pl.BlockSpec((slab, cols, deep), lambda i: (i, 0, 0))
    kind = jnp.float32
    return pl.pallas_call(
        spread_kernel,
        grid=(rows // slab,),
        in_specs=[whole_smem(), whole_smem(), whole_smem(), vector, vector, scalar, scalar] + [pl.BlockSpec(memory_space=pl.ANY)] * 2,
        out_specs=[whole_vmem()] * 5,
        compiler_params=limited(),
        out_shape=[
            pltpu.HBM((comps * freqs * 2, 24, cols), kind),
            room((2, cols, deep)),
            room((2, cols, deep)),
            room((2, rows, deep)),
            room((2, rows, deep)),
        ],
        scratch_shapes=[
            room((rows, 16, LANES)), room((3, rows, LANES)), room((2, LANES)),
            room(spectrum_real.shape), room(spectrum_imag.shape), pltpu.SemaphoreType.DMA((2,)),
        ],
        name="spread",
    )(edge, cosine, sine, *(far_kept(a) for a in (electric, magnetic, retention, coupling, spectrum_real, spectrum_imag)))


def split_high(value):
    high = value.astype(jnp.bfloat16)
    return high, (value - high.astype(jnp.float32)).astype(jnp.bfloat16)


def dot(a, b):
    return jnp.dot(a, b, preferred_element_type=jnp.float32)


def along_y_kernel(at, cosine, sine, got, high, low, mine, other, lines):
    along_x, along_y = got.shape[0], got.shape[1]
    blocks = along_x * along_y
    half = at[0] % 2
    freq = (at[0] // 2) % cosine.shape[0]
    weight_real = cosine[freq]
    weight_imag = -sine[freq]
    is_last = jnp.where(half == 1, 1.0, 0.0)
    is_first = jnp.where(half == 0, 1.0, 0.0)

    packed = jnp.concatenate([got[x, :, 20, :] for x in range(along_x)], axis=0)
    block = spot((blocks, LANES), 0)
    lane = spot((blocks, LANES), 1)
    inner = block % along_y
    rows = 16

    def lines_at(value, which):
        return jnp.where(lane < rows, moved(value, -which * rows, 1), 0.0)

    from_right = jnp.where(inner == along_y - 1, 0.0, moved(packed, -1, 0))
    from_left = jnp.where(inner == 0, 0.0, moved(packed, 1, 0))
    comp = at[0] // (2 * cosine.shape[0])
    right_up = jnp.where((block >= along_y) & (comp == 1), moved(from_right, along_y, 0), 0.0)
    left_down = jnp.where((block < blocks - along_y) & (comp == 0), moved(from_left, -along_y, 0), 0.0)
    from_right = lines_at(from_right, 0) + jnp.where(lane == 0, moved(right_up, -4 * rows, 1), 0.0)
    from_left = lines_at(from_left, 1) + jnp.where(lane == rows - 1, moved(left_down, -3 * rows - 1, 1), 0.0)
    last_col = lines_at(packed, 2) * from_right
    first_col = lines_at(packed, 3) * from_left
    pad = jnp.zeros((LANES - 2 * blocks, LANES), jnp.float32)
    upright = jnp.concatenate([last_col, first_col, pad], axis=0).T
    cols = jnp.where(half == 0, upright[0:8], upright[8:16])

    low_row = spot((SUBLANES, LANES), 0)
    low_lane = spot((SUBLANES, LANES), 1)
    for x in range(along_x):
        for y in range(along_y):
            here = x * along_y + y
            delta = jnp.where(low_lane == LANES - 1, moved(cols, LANES - 1 - here, 1), 0.0)
            delta = delta + jnp.where(low_lane == 0, moved(cols, -blocks - here, 1), 0.0)
            if x + 1 < along_x:
                row = got[x, y, 18:19, :] * got[x + 1, y, 16:17, :] * is_last
                delta = delta + jnp.where(low_row == SUBLANES - 1, row, 0.0)
            if x > 0:
                row = got[x, y, 19:20, :] * got[x - 1, y, 17:18, :] * is_first
                delta = delta + jnp.where(low_row == 0, row, 0.0)
            span = slice(y * LANES, (y + 1) * LANES)
            lines[x * 16 : x * 16 + 8, span] = got[x, y, 0:8, :] + weight_real * delta
            lines[x * 16 + 8 : x * 16 + 16, span] = got[x, y, 8:16, :] + weight_imag * delta

    lines_high, lines_low = split_high(lines[...])
    total = dot(lines_high, high[...]) + (dot(lines_low, high[...]) + dot(lines_high, low[...]))
    waves = total.shape[1] // 2
    piece = waves // 2
    for x in range(along_x):
        top = total[x * 16 : x * 16 + 8]
        bottom = total[x * 16 + 8 : x * 16 + 16]
        new_real = top[:, :waves] + bottom[:, waves:]
        new_imag = bottom[:, :waves] - top[:, waves:]
        span = slice(x * 8, x * 8 + 8)
        mine[span, :piece] = jnp.where(half == 0, new_real[:, :piece], new_real[:, piece:])
        mine[span, piece:] = jnp.where(half == 0, new_imag[:, :piece], new_imag[:, piece:])
        other[span, :piece] = jnp.where(half == 0, new_real[:, piece:], new_real[:, :piece])
        other[span, piece:] = jnp.where(half == 0, new_imag[:, piece:], new_imag[:, :piece])


def along_y_sums(place, cosine, sine, got, cols, along_x, along_y):
    wide = WAVES // along_y
    order = np.arange(WAVES).reshape(along_y, 2, wide // 2).transpose(1, 0, 2).reshape(-1)
    cos_y, sin_y = wave_tables(WAVES, cols * along_y)
    high, low = in_two(np.concatenate([cos_y[order].T, sin_y[order].T], axis=1))
    shape = room((along_x * 8, WAVES))
    return pl.pallas_call(
        along_y_kernel,
        in_specs=[whole_smem()] * 3 + [whole_vmem()] * 3,
        out_specs=[whole_vmem()] * 2,
        out_shape=[shape, shape],
        scratch_shapes=[room((along_x * 16, along_y * LANES))],
        compiler_params=limited(),
        name="along_y",
    )(place, cosine, sine, kept(got.reshape(along_x, along_y, 24, cols)), kept(high), kept(low))


def along_x_kernel(along_x, at, mine, other, high, low, out):
    half = at[0] % 2
    lines = jnp.concatenate(
        [jnp.where(half == 0, mine[...], other[...]), jnp.where(half == 0, other[...], mine[...])], axis=0
    )
    lines_high, lines_low = split_high(lines)
    total = dot(high[...], lines_high) + (dot(high[...], lines_low) + dot(low[...], lines_high))
    waves = total.shape[0] // 2
    piece = total.shape[1] // 2
    far = (
        total[:waves, :piece] + total[waves:, piece:],
        total[:waves, piece:] - total[waves:, :piece],
    )
    tall = waves // along_x
    stacks = tall // SUBLANES
    along_y = out.shape[0] // along_x
    wide = piece // along_y
    lane = spot((SUBLANES, LANES), 1)
    for x in range(along_x):
        for part in range(2):
            tiles = [far[part][x * tall + q * 8 : x * tall + q * 8 + 8] for q in range(stacks)]
            for y in range(along_y):
                block = None
                for q in range(stacks):
                    tile = moved(tiles[q], (q - y) * wide, 1)
                    block = tile if block is None else jnp.where(lane < q * wide, block, tile)
                out[x * along_y + y, part * 8 : part * 8 + 8] = block


def along_x_sums(place, mine, other, rows, scale, along_x, devices):
    cos_x, sin_x = wave_tables(WAVES, rows * along_x)
    table = np.concatenate([cos_x, sin_x], axis=0) * scale
    table = table.reshape(2 * WAVES, along_x, 2, 8).transpose(0, 2, 1, 3).reshape(2 * WAVES, rows * along_x)
    high, low = in_two(table)
    return pl.pallas_call(
        lambda *refs: along_x_kernel(along_x, *refs),
        in_specs=[whole_smem()] + [whole_vmem()] * 4,
        out_specs=whole_vmem(),
        out_shape=pltpu.HBM((devices, 16, LANES), jnp.float32),
        compiler_params=limited(),
        name="along_x",
    )(place, kept(mine), kept(other), kept(high), kept(low))


def placed_kernel(got, out):
    planes, tall, wide = out.shape[1:]
    piece = wide // 2
    lane = spot((SUBLANES, LANES), 1)
    for plane in range(planes):
        for part in range(2):
            first = got[2 * plane, part * 8 : part * 8 + 8]
            second = got[2 * plane + 1, part * 8 : part * 8 + 8]
            for q in range(tall // SUBLANES):
                tile = jnp.where(lane < piece, moved(first, -q * piece, 1), moved(second, piece - q * piece, 1))
                out[part, plane, q * 8 : q * 8 + 8, :] = tile[:, :wide]


def placed_far(got, comps, freqs, tall, wide):
    far = pl.pallas_call(
        placed_kernel,
        in_specs=[whole_vmem()],
        out_specs=whole_vmem(),
        out_shape=jax.ShapeDtypeStruct((2, comps * freqs, tall, wide), jnp.float32),
        compiler_params=limited(),
        name="placed",
    )(kept(got))
    return far.reshape(2, comps, freqs, tall, wide)


def yee_kernel(
    edge, place, cosine, sine, elec, ahead, magn, ret, coup, rows_elec, rows_magn, cols_elec, cols_magn, got,
    real, imag, new_elec, new_magn, new_real, new_imag, carried, tops,
):
    step = pl.program_id(0)
    steps = pl.num_programs(0)
    deep = elec.shape[1]
    inner_x = edge[0]
    inner_y = edge[1]
    corner_up = got[place[1], 21:22, :] * edge[2]
    corner_down = got[place[2], 22:23, :] * edge[3]
    row = spot((LANES, LANES), 0)
    lane = spot((LANES, LANES), 1)

    @pl.when(step == 0)
    def _():
        spare = jnp.where(row == LANES - 1, curl_step * corner_down, 0.0)
        carried[0] = (rows_magn[0] + curl_step * elec[2, 0]) * inner_x
        carried[1] = (rows_magn[1] - curl_step * elec[1, 0] + spare) * inner_x

    at_end = step == steps - 1
    for at in range(deep):
        here = pl.ds(step * deep + at, 1)
        ex, ey, ez = elec[0, at], elec[1, at], elec[2, at]
        if at + 1 < deep:
            ey_next, ez_next = elec[1, at + 1], elec[2, at + 1]
        else:
            ey_next = jnp.where(at_end, rows_elec[0], ahead[1, 0])
            ez_next = jnp.where(at_end, rows_elec[1], ahead[2, 0])
        hx = magn[0, at] - curl_step * ((after(ez, 0, cols_elec[1, here, :]) - ez) - (after(ey, 1) - ey))
        hy = magn[1, at] - curl_step * ((after(ex, 1) - ex) - (ez_next - ez))
        hz = magn[2, at] - curl_step * ((ey_next - ey) - (after(ex, 0, cols_elec[0, here, :]) - ex))
        new_magn[0, at] = hx
        new_magn[1, at] = hy
        new_magn[2, at] = hz
        side_x = (cols_magn[0, here, :] - curl_step * ez[0:1]) * inner_y
        side_z = cols_magn[1, here, :] + curl_step * ex[0:1]
        if at + 1 == deep:
            side_z = side_z - jnp.where(at_end, curl_step * corner_up, 0.0)
        side_z = side_z * inner_y
        keep, gain = ret[at], coup[at]
        new_x = keep * ex + gain * ((hz - before(hz, 0, side_z)) - (hy - before(hy, 1)))
        new_y = keep * ey + gain * ((hx - before(hx, 1)) - (hz - carried[1]))
        new_z = keep * ez + gain * ((hy - carried[0]) - (hx - before(hx, 0, side_x)))
        new_elec[0, at] = new_x
        new_elec[1, at] = new_y
        new_elec[2, at] = new_z
        carried[0] = hy
        carried[1] = hz
        packed = None
        for which, value in enumerate((new_x, new_y, hx, hy)):
            turned = moved(value, which - TOP_PLANE, 1)
            packed = turned if packed is None else jnp.where(lane < which, packed, turned)
        tops[step * deep + at] = packed.T[0:SUBLANES]

    @pl.when(at_end)
    def _():
        for comp in range(4):
            tangent = tops[:, comp, :]
            for freq in range(real.shape[1]):
                new_real[comp, freq] = real[comp, freq] + tangent * cosine[freq]
                new_imag[comp, freq] = imag[comp, freq] - tangent * sine[freq]


def yee(edge, place, cosine, sine, electric, magnetic, retention, coupling, halos, got, spectrum_real, spectrum_imag):
    _, rows, cols, deep = electric.shape
    slab = 2
    steps = rows // slab
    vector = pl.BlockSpec((3, slab, cols, deep), lambda i: (0, i, 0, 0))
    ahead = pl.BlockSpec((3, 1, cols, deep), lambda i: (0, jnp.minimum((i + 1) * slab, rows - 1), 0, 0))
    scalar = pl.BlockSpec((slab, cols, deep), lambda i: (i, 0, 0))
    kind = jnp.float32
    return pl.pallas_call(
        yee_kernel,
        grid=(steps,),
        in_specs=[whole_smem()] * 4 + [vector, ahead, vector, scalar, scalar] + [whole_vmem()] * 7,
        compiler_params=limited(),
        out_specs=[vector, vector, whole_vmem(), whole_vmem()],
        out_shape=[
            jax.ShapeDtypeStruct(electric.shape, kind),
            jax.ShapeDtypeStruct(magnetic.shape, kind),
            jax.ShapeDtypeStruct(spectrum_real.shape, kind),
            jax.ShapeDtypeStruct(spectrum_imag.shape, kind),
        ],
        scratch_shapes=[pltpu.VMEM((2, cols, deep), kind), pltpu.VMEM((rows, SUBLANES, LANES), kind)],
        cost_estimate=pl.CostEstimate(flops=60 * electric.size, bytes_accessed=20 * electric.size, transcendentals=0),
        name="yee",
    )(
        edge, place, cosine, sine,
        *(far_kept(a) for a in (electric, electric, magnetic, retention, coupling)),
        *(kept(halo) for halo in halos), kept(got), far_kept(spectrum_real), far_kept(spectrum_imag),
    )


def tiled_step(electric, magnetic, retention, coupling, spectrum_real, spectrum_imag, phases):
    comps, freqs, rows, cols = spectrum_real.shape
    along_x, along_y = lax.axis_size("gx"), lax.axis_size("gy")
    devices = along_x * along_y
    cosine, sine = jnp.cos(phases), jnp.sin(phases)
    at_x, at_y = lax.axis_index("gx"), lax.axis_index("gy")
    here = lax.axis_index(BOTH)
    inner = (at_x > 0, at_y > 0, (at_x + 1 < along_x) & (at_y > 0), (at_x > 0) & (at_y + 1 < along_y))
    edge = jnp.stack(inner).astype(jnp.float32)
    up, down = jnp.minimum(here + along_y - 1, devices - 1), jnp.maximum(here - along_y + 1, 0)
    place = jnp.stack([here, up, down]).astype(jnp.int32)
    sent, rows_elec, rows_magn, cols_elec, cols_magn = spread(
        edge, electric, magnetic, retention, coupling, spectrum_real, spectrum_imag, cosine, sine
    )
    got = lax.all_to_all(sent, BOTH, split_axis=0, concat_axis=0, tiled=True)
    halos = (
        passed_along(rows_elec, "gx", -1),
        passed_along(rows_magn, "gx", 1),
        passed_along(cols_elec, "gy", -1),
        passed_along(cols_magn, "gy", 1),
    )
    mine, other = along_y_sums(place, cosine, sine, got, cols, along_x, along_y)
    other = swapped(other, 1)
    scale = 1.0 / math.sqrt(rows * along_x * cols * along_y)
    far = along_x_sums(place, mine, other, rows, scale, along_x, devices)
    far = lax.all_to_all(far, BOTH, split_axis=0, concat_axis=0, tiled=True)
    next_electric, next_magnetic, next_real, next_imag = yee(
        edge, place, cosine, sine, electric, magnetic, retention, coupling, halos, got,
        spectrum_real, spectrum_imag,
    )
    far_field = placed_far(far, comps, freqs, WAVES // along_x, WAVES // along_y)
    return (next_electric, next_magnetic, next_real, next_imag, far_field)


def per_device(*arrays):
    comps, freqs, rows, cols = arrays[4].shape
    depth = arrays[0].shape[3]
    along_x, along_y = lax.axis_size("gx"), lax.axis_size("gy")
    wide, tall = WAVES // along_y, WAVES // along_x
    fits = (
        comps == 4
        and along_x * along_y == 2 * comps * freqs
        and (rows, cols, depth) == (2 * SUBLANES, LANES, LANES)
        and WAVES == 2 * LANES
        and (wide // 2) * (tall // SUBLANES) == LANES
        and 0 < TOP_PLANE < depth - 1
    )
    return tiled_step(*arrays) if fits else general_step(*arrays)


def solution(mesh):
    placed = (
        P(None, "gx", "gy", None),
        P(None, "gx", "gy", None),
        P("gx", "gy", None),
        P("gx", "gy", None),
        P(None, None, "gx", "gy"),
        P(None, None, "gx", "gy"),
        P(),
    )
    return jax.shard_map(
        per_device,
        mesh=mesh,
        in_specs=placed,
        out_specs=(
            P(None, "gx", "gy", None),
            P(None, "gx", "gy", None),
            P(None, None, "gx", "gy"),
            P(None, None, "gx", "gy"),
            P(None, None, None, "gx", "gy"),
        ),
        check_vma=False,
    )
```

```python
import math

import jax
import jax.numpy as jnp
import numpy as np
from jax import lax
from jax.experimental import pallas as pl
from jax.experimental.pallas import tpu as pltpu
from jax.sharding import PartitionSpec as P


WAVES = 256
TOP_PLANE = 111
BOTH = ("gx", "gy")
LANES = 128
SUBLANES = 8

curl_step = 0.5


def passed_along(value, axis, by):
    devices = lax.axis_size(axis)
    pairs = [(i, i + by) for i in range(devices) if 0 <= i + by < devices]
    return lax.ppermute(value, axis, pairs)


def traded(value, axis, odd):
    devices = lax.axis_size(axis)
    pairs = [(i, i + 1 if i % 2 == odd else i - 1) for i in range(devices)]
    return lax.ppermute(value, axis, [(i, to) for i, to in pairs if 0 <= to < devices])


def swapped(value, by):
    devices = lax.axis_size(BOTH)
    return lax.ppermute(value, BOTH, [(i, i ^ by) for i in range(devices)])


def wave_tables(number, extent):
    wave = 2 * np.arange(number) + 1 - number
    angles = (wave[:, None] * np.arange(extent)[None, :] % (4 * number)) * (math.pi / (2 * number))
    return np.cos(angles), np.sin(angles)


def in_two(table):
    high = table.astype(np.float32).astype(jnp.bfloat16)
    low = (table - high.astype(np.float64)).astype(np.float32).astype(jnp.bfloat16)
    return jnp.asarray(high), jnp.asarray(low)


def forward_diff(values, along):
    padded = jnp.pad(values, [(0, 1) if which == along else (0, 0) for which in range(values.ndim)])
    return lax.slice_in_dim(padded, 1, values.shape[along] + 1, axis=along) - values


def backward_diff(values, along):
    padded = jnp.pad(values, [(1, 0) if which == along else (0, 0) for which in range(values.ndim)])
    return values - lax.slice_in_dim(padded, 0, values.shape[along], axis=along)


def ahead_diff(values, border, along):
    upper = lax.slice_in_dim(values, 1, values.shape[along], axis=along)
    return jnp.concatenate([upper, border], axis=along) - values


def behind_diff(values, border, along):
    lower = lax.slice_in_dim(values, 0, values.shape[along] - 1, axis=along)
    return values - jnp.concatenate([border, lower], axis=along)


def far_of(next_real, next_imag):
    highest = lax.Precision.HIGHEST
    comps, freqs, rows, cols = next_real.shape
    along_x, along_y = lax.axis_size("gx"), lax.axis_size("gy")
    devices = along_x * along_y
    planes = comps * freqs
    share = devices // planes
    part_rows = rows // share
    wide = WAVES // along_y
    part_wide = wide // share
    tall = WAVES // along_x
    place = lax.axis_index(BOTH) % share

    both = jnp.stack([next_real, next_imag]).reshape(2, planes, share, part_rows, cols)
    both = both.transpose(1, 2, 0, 3, 4).reshape(devices, 2, part_rows, cols)
    got = lax.all_to_all(both, BOTH, split_axis=0, concat_axis=0, tiled=True)
    got = got.reshape(along_x, along_y, 2, part_rows, cols)

    cos_y, sin_y = (table.astype(np.float32) for table in wave_tables(WAVES, cols * along_y))
    order_k = np.arange(WAVES).reshape(along_y, share, part_wide).transpose(1, 0, 2).reshape(-1)
    cos_y = cos_y[order_k].reshape(share, -1, along_y, cols)
    sin_y = sin_y[order_k].reshape(share, -1, along_y, cols)
    with_cos = jnp.einsum("gbirc,skbc->sigrk", got, cos_y, precision=highest)
    with_sin = jnp.einsum("gbirc,skbc->sigrk", got, sin_y, precision=highest)
    partial = jnp.stack([with_cos[:, 0] + with_sin[:, 1], with_cos[:, 1] - with_sin[:, 0]], axis=1)

    pieces = []
    for by in range(share):
        piece = lax.dynamic_index_in_dim(partial, place ^ by, 0, keepdims=False)
        pieces.append(piece if by == 0 else swapped(piece, by))
    pieces = jnp.stack(pieces)
    partial = jnp.stack(
        [lax.dynamic_index_in_dim(pieces, place ^ s, 0, keepdims=False) for s in range(share)]
    )

    cos_x, sin_x = (table.astype(np.float32) for table in wave_tables(WAVES, rows * along_x))
    cos_x = cos_x.reshape(WAVES, along_x, share, part_rows)
    sin_x = sin_x.reshape(WAVES, along_x, share, part_rows)
    with_cos = jnp.einsum("jgsr,sigrk->ijk", cos_x, partial, precision=highest)
    with_sin = jnp.einsum("jgsr,sigrk->ijk", sin_x, partial, precision=highest)
    far = jnp.stack([with_cos[0] + with_sin[1], with_cos[1] - with_sin[0]])
    far = far * (1.0 / math.sqrt(rows * along_x * cols * along_y))

    far = far.reshape(2, along_x, tall, along_y, part_wide).transpose(1, 3, 0, 2, 4)
    far = far.reshape(devices, 2, tall, part_wide)
    far = lax.all_to_all(far, BOTH, split_axis=0, concat_axis=0, tiled=True)
    far = far.reshape(comps, freqs, share, 2, tall, part_wide).transpose(3, 0, 1, 4, 2, 5)
    return far.reshape(2, comps, freqs, tall, wide)


def general_step(electric, magnetic, retention, coupling, spectrum_real, spectrum_imag, phases):
    elec_x, elec_y, elec_z = (electric[0], electric[1], electric[2])
    rows_elec = passed_along(electric[1:3, 0:1], "gx", -1)
    cols_elec = passed_along(electric[0:3:2, :, 0:1], "gy", -1)
    mag_x = magnetic[0] - curl_step * (
        ahead_diff(elec_z, cols_elec[1], 1) - forward_diff(elec_y, 2)
    )
    mag_y = magnetic[1] - curl_step * (
        forward_diff(elec_x, 2) - ahead_diff(elec_z, rows_elec[1], 0)
    )
    mag_z = magnetic[2] - curl_step * (
        ahead_diff(elec_y, rows_elec[0], 0) - ahead_diff(elec_x, cols_elec[0], 1)
    )
    next_magnetic = jnp.stack([mag_x, mag_y, mag_z])
    rows_magn = passed_along(next_magnetic[1:3, -1:], "gx", 1)
    cols_magn = passed_along(next_magnetic[0:3:2, :, -1:], "gy", 1)
    new_x = retention * elec_x + coupling * (
        behind_diff(mag_z, cols_magn[1], 1) - backward_diff(mag_y, 2)
    )
    new_y = retention * elec_y + coupling * (
        backward_diff(mag_x, 2) - behind_diff(mag_z, rows_magn[1], 0)
    )
    new_z = retention * elec_z + coupling * (
        behind_diff(mag_y, rows_magn[0], 0) - behind_diff(mag_x, cols_magn[0], 1)
    )
    next_electric = jnp.stack([new_x, new_y, new_z])
    tangent = jnp.stack(
        [
            new_x[:, :, TOP_PLANE],
            new_y[:, :, TOP_PLANE],
            mag_x[:, :, TOP_PLANE],
            mag_y[:, :, TOP_PLANE],
        ]
    )
    next_real = spectrum_real + tangent[:, None] * jnp.cos(phases)[None, :, None, None]
    next_imag = spectrum_imag - tangent[:, None] * jnp.sin(phases)[None, :, None, None]
    return (next_electric, next_magnetic, next_real, next_imag, far_of(next_real, next_imag))


def spot(shape, axis):
    return lax.broadcasted_iota(jnp.int32, shape, axis)


def moved(value, by, axis):
    by = by % value.shape[axis]
    return value if by == 0 else pltpu.roll(value, by, axis)


def after(value, axis, border=0.0):
    size = value.shape[axis]
    return jnp.where(spot(value.shape, axis) == size - 1, border, moved(value, -1, axis))


def before(value, axis, border=0.0):
    return jnp.where(spot(value.shape, axis) == 0, border, moved(value, 1, axis))


def whole_vmem():
    return pl.BlockSpec(memory_space=pltpu.VMEM)


def kept(value):
    return pltpu.with_memory_space_constraint(value, pltpu.VMEM)


def far_kept(value):
    return pltpu.with_memory_space_constraint(value, pltpu.HBM)


def room(shape, dtype=jnp.float32):
    return pltpu.VMEM(shape, dtype)


def limited(size=24):
    return pltpu.CompilerParams(vmem_limit_bytes=size * 1024 * 1024)


PLACES = LANES // SUBLANES
PICKED = ((0, -1, 3), (1, -1, 3), (2, -1, 2), (3, -1, 2), (4, -1, 2), (5, 0, 1), (6, 0, 1), (7, 0, 1))


def arrivals(chunk, deep, sources, targets, arrived):
    span = pl.ds(chunk * deep, deep)
    pairs = []
    for source, target in zip(sources, targets):
        lead = [(i, span) for i in range(source.shape[0])] if len(source.shape) == 4 else [(span,)]
        pairs += [(source.at[at], target.at[at]) for at in lead]
    return [pltpu.make_async_copy(*pair, arrived.at[chunk, i]) for i, pair in enumerate(pairs)]


def spread_kernel(
    phases_far, elec_far, magn_far, ret_far, coup_far, real_far, imag_far,
    out_far, rows_first, rows_second, cols_first, cols_second, trig, known,
    elec, magn, ret, coup, cols_elec, cols_magn, planes, ends, out, real, imag, phases, arrived, small, leaving,
):
    chunks = arrived.shape[0]
    rows = ret.shape[0]
    deep = rows // chunks
    freqs = real.shape[1]

    def copies(chunk):
        return arrivals(chunk, deep, (elec_far, magn_far, ret_far, coup_far), (elec, magn, ret, coup), arrived)

    extras = [
        pltpu.make_async_copy(phases_far, phases, small.at[0]),
        pltpu.make_async_copy(real_far, real, small.at[1]),
        pltpu.make_async_copy(imag_far, imag, small.at[2]),
    ]
    extras[0].start()
    for chunk in range(chunks):
        for copy in copies(chunk):
            copy.start()
    extras[1].start()
    extras[2].start()
    extras[0].wait()
    turn_row = spot((SUBLANES, LANES), 0)
    angle = jnp.zeros((SUBLANES, LANES), jnp.float32)
    for freq in range(freqs):
        angle = jnp.where(turn_row == freq, phases[freq], angle)
    trig[0] = jnp.cos(angle)
    trig[1] = jnp.sin(angle)
    lane = spot((LANES, LANES), 1)

    packed = None
    for at in range(rows):
        if at % deep == 0:
            for copy in copies(at // deep):
                copy.wait()
        arrays = [elec[0, at], elec[1, at], elec[2, at], magn[0, at], magn[1, at], magn[2, at], ret[at], coup[at]]
        start = at % SUBLANES * PLACES
        for which, first, count in PICKED:
            turned = moved(arrays[which], start - TOP_PLANE - first, 1)
            packed = turned if packed is None else jnp.where(lane < start, packed, turned)
            start += count
        if at % SUBLANES == SUBLANES - 1:
            planes[at // SUBLANES] = packed.T
            packed = None
        ends[0, at : at + 1, :] = elec[0, at, -1:, :]
        ends[1, at : at + 1, :] = elec[1, at, -1:, :]
        ends[2, at : at + 1, :] = magn[2, at, -1:, :]
        cols_elec[0, at : at + 1, :] = elec[0, at, 0:1, :]
        cols_elec[1, at : at + 1, :] = elec[2, at, 0:1, :]
        line = elec[1, at, -1:, :]
        cols_magn[0, at : at + 1, :] = (
            magn[0, at, -1:, :] + curl_step * elec[2, at, -1:, :] + curl_step * (after(line, 1) - line)
        )

    last = rows - 1
    ex, ey, ez = elec[0, last], elec[1, last], elec[2, last]
    upward = (elec[1, 0], elec[2, 0])
    downward = (
        magn[1, last] - curl_step * (after(ex, 1) - ex) - curl_step * ez,
        magn[2, last] + curl_step * ey + curl_step * (after(ex, 0) - ex),
    )
    even = lax.axis_index("gx") % 2 == 0
    for i in range(2):
        rows_first[i] = jnp.where(even, downward[i], upward[i])
        rows_second[i] = jnp.where(even, upward[i], downward[i])
    end_x, end_y, end_z = ends[0], ends[1], ends[2]
    cols_magn[1] = end_z - curl_step * (after(end_y, 0) - end_y) - curl_step * end_x
    even = lax.axis_index("gy") % 2 == 0
    cols_first[...] = jnp.where(even, cols_magn[...], cols_elec[...])
    cols_second[...] = jnp.where(even, cols_elec[...], cols_magn[...])
    corner_up, corner_down = elec[1, 0, -1:, :], elec[0, last, 0:1, :]

    if rows:
        ex_m, ex_p, ex_q, ey_m, ey_p, ey_q, ez_m, ez_p, hx_m, hx_p, hy_m, hy_p, hz_p, keep, gain = (
            jnp.concatenate([planes[group, pl.ds(which, SUBLANES, stride=PLACES), :] for group in range(rows // SUBLANES)])
            for which in range(15)
        )
        hx_p = hx_p - curl_step * ((after(ez_p, 1) - ez_p) - (ey_q - ey_p))
        hx_m = hx_m - curl_step * ((after(ez_m, 1) - ez_m) - (ey_p - ey_m))
        hy_p = hy_p - curl_step * ((ex_q - ex_p) - (after(ez_p, 0) - ez_p))
        hy_m = hy_m - curl_step * ((ex_p - ex_m) - (after(ez_m, 0) - ez_m))
        hz_p = hz_p - curl_step * ((after(ey_p, 0) - ey_p) - (after(ex_p, 1) - ex_p))
        edge_x = jnp.where(lax.axis_index("gx") > 0, curl_step, 0.0)
        edge_y = jnp.where(lax.axis_index("gy") > 0, curl_step, 0.0)
        tangent = (
            keep * ex_p + gain * ((hz_p - before(hz_p, 1, edge_y * ex_p)) - (hy_p - hy_m)),
            keep * ey_p + gain * ((hx_p - hx_m) - (hz_p - before(hz_p, 0, -edge_x * ey_p))),
            hx_p,
            hy_p,
        )
        for which, value in enumerate((*tangent, gain)):
            known[which] = value
        ez_jump = curl_step * (ez_p - ez_m)
        push = -curl_step * ey_p
        none = jnp.zeros_like(ex_p)
        one = jnp.ones_like(ex_p)
        row_up = (push - before(push, 1) - ez_jump, -push, none, curl_step * ez_p)
        row_down = (none, hz_p, none, none)
        col_left = (
            curl_step * ex_p,
            -ez_jump - curl_step * ex_p + before(curl_step * ex_p, 0),
            -curl_step * ez_p,
            none,
        )
        col_right = (-hz_p, none, none, none)
        wide = lax.broadcasted_iota(jnp.int32, (LANES, LANES), 1)
        tall = lax.broadcasted_iota(jnp.int32, (SUBLANES, LANES), 0)
        lanes = lax.broadcasted_iota(jnp.int32, (SUBLANES, LANES), 1)
        pad = jnp.zeros((LANES - rows, LANES), jnp.float32)

        def upright(lines):
            block = None
            for which, (value, column) in enumerate(lines):
                value = moved(value, which - column, 1)
                block = value if block is None else jnp.where(wide[0:rows] < which, block, value)
            return jnp.concatenate([block, pad], axis=0).T[0:SUBLANES]

        end = LANES - 1
        extras[1].wait()
        extras[2].wait()
        departures = []
        for comp in range(4):
            factor = gain if comp < 2 else one
            columns = upright([(col_left[comp], 0), (col_right[comp], end), (factor, end), (factor, 0)])
            columns = sum(moved(columns[which : which + 1], which * rows, 1) for which in range(4))
            if comp < 2:
                spare = moved(-push[0:1], -end, 1) if comp == 0 else curl_step * ex_p[rows - 1 :]
                columns = jnp.where(lanes[0:1] == 4 * rows, moved(spare, 4 * rows, 1), columns)
            extra = jnp.where(tall == 0, row_up[comp][0:1], 0.0)
            extra = jnp.where(tall == 1, row_down[comp][rows - 1 :], extra)
            extra = jnp.where(tall == 2, factor[rows - 1 :], extra)
            extra = jnp.where(tall == 3, factor[0:1], extra)
            extra = jnp.where(tall == 4, columns, extra)
            extra = jnp.where(tall == 5, corner_up, extra)
            extra = jnp.where(tall == 6, corner_down, extra)
            for freq in range(freqs):
                new_real = real[comp, freq] + tangent[comp] * trig[0, freq : freq + 1, :]
                new_imag = imag[comp, freq] - tangent[comp] * trig[1, freq : freq + 1, :]
                for half in range(2):
                    to = (comp * freqs + freq) * 2 + half
                    out[to, 0:8] = new_real[half * 8 : half * 8 + 8]
                    out[to, 8:16] = new_imag[half * 8 : half * 8 + 8]
                    out[to, 16:24] = extra
            span = pl.ds(comp * freqs * 2, freqs * 2)
            departures.append(pltpu.make_async_copy(out.at[span], out_far.at[span], leaving.at[comp]))
            departures[-1].start()
        for departure in departures:
            departure.wait()


def spread(electric, magnetic, retention, coupling, spectrum_real, spectrum_imag, phases):
    _, rows, cols, deep = electric.shape
    comps, freqs = spectrum_real.shape[:2]
    chunks = 4
    sent = (comps * freqs * 2, 24, cols)
    inputs = (phases, electric, magnetic, retention, coupling, spectrum_real, spectrum_imag)
    return pl.pallas_call(
        spread_kernel,
        in_specs=[pl.BlockSpec(memory_space=pl.ANY)] * 7,
        out_specs=[pl.BlockSpec(memory_space=pl.ANY)] + [whole_vmem()] * 6,
        compiler_params=limited(),
        out_shape=[
            pltpu.HBM(sent, jnp.float32),
            room((2, cols, deep)),
            room((2, cols, deep)),
            room((2, rows, deep)),
            room((2, rows, deep)),
            room((2, SUBLANES, LANES)),
            room((comps + 1, rows, cols)),
        ],
        scratch_shapes=[
            room(electric.shape),
            room(magnetic.shape),
            room(retention.shape),
            room(coupling.shape),
            room((2, rows, deep)),
            room((2, rows, deep)),
            room((rows // SUBLANES, LANES, LANES)),
            room((3, rows, LANES)),
            room(sent),
            room(spectrum_real.shape),
            room(spectrum_imag.shape),
            pltpu.SMEM((freqs,), jnp.float32),
            pltpu.SemaphoreType.DMA((chunks, 8)),
            pltpu.SemaphoreType.DMA((3,)),
            pltpu.SemaphoreType.DMA((comps,)),
        ],
        name="spread",
    )(*(far_kept(value) for value in inputs))


def split_high(value):
    high = value.astype(jnp.bfloat16)
    return high, (value - high.astype(jnp.float32)).astype(jnp.bfloat16)


def dot(a, b):
    return jnp.dot(a, b, preferred_element_type=jnp.float32)


def along_y_kernel(got, trig, high, low, mine, other, lines):
    along_x, along_y = got.shape[0], got.shape[1]
    blocks = along_x * along_y
    at = lax.axis_index(BOTH)
    half = at % 2
    freqs = got.shape[0] * got.shape[1] // 8
    freq = (at // 2) % freqs
    weight_real = trig[0, pl.ds(freq, 1), :]
    weight_imag = -trig[1, pl.ds(freq, 1), :]
    is_last = jnp.where(half == 1, 1.0, 0.0)
    is_first = jnp.where(half == 0, 1.0, 0.0)

    packed = jnp.concatenate([got[x, :, 20, :] for x in range(along_x)], axis=0)
    block = spot((blocks, LANES), 0)
    lane = spot((blocks, LANES), 1)
    inner = block % along_y
    rows = 16

    def lines_at(value, which):
        return jnp.where(lane < rows, moved(value, -which * rows, 1), 0.0)

    from_right = jnp.where(inner == along_y - 1, 0.0, moved(packed, -1, 0))
    from_left = jnp.where(inner == 0, 0.0, moved(packed, 1, 0))
    comp = at // (2 * freqs)
    right_up = jnp.where((block >= along_y) & (comp == 1), moved(from_right, along_y, 0), 0.0)
    left_down = jnp.where((block < blocks - along_y) & (comp == 0), moved(from_left, -along_y, 0), 0.0)
    from_right = lines_at(from_right, 0) + jnp.where(lane == 0, moved(right_up, -4 * rows, 1), 0.0)
    from_left = lines_at(from_left, 1) + jnp.where(lane == rows - 1, moved(left_down, -3 * rows - 1, 1), 0.0)
    last_col = lines_at(packed, 2) * from_right
    first_col = lines_at(packed, 3) * from_left
    pad = jnp.zeros((LANES - 2 * blocks, LANES), jnp.float32)
    upright = jnp.concatenate([last_col, first_col, pad], axis=0).T
    cols = jnp.where(half == 0, upright[0:8], upright[8:16])

    low_row = spot((SUBLANES, LANES), 0)
    low_lane = spot((SUBLANES, LANES), 1)
    for x in range(along_x):
        for y in range(along_y):
            here = x * along_y + y
            delta = jnp.where(low_lane == LANES - 1, moved(cols, LANES - 1 - here, 1), 0.0)
            delta = delta + jnp.where(low_lane == 0, moved(cols, -blocks - here, 1), 0.0)
            if x + 1 < along_x:
                row = got[x, y, 18:19, :] * got[x + 1, y, 16:17, :] * is_last
                delta = delta + jnp.where(low_row == SUBLANES - 1, row, 0.0)
            if x > 0:
                row = got[x, y, 19:20, :] * got[x - 1, y, 17:18, :] * is_first
                delta = delta + jnp.where(low_row == 0, row, 0.0)
            span = slice(y * LANES, (y + 1) * LANES)
            lines[x * 16 : x * 16 + 8, span] = got[x, y, 0:8, :] + weight_real * delta
            lines[x * 16 + 8 : x * 16 + 16, span] = got[x, y, 8:16, :] + weight_imag * delta

    lines_high, lines_low = split_high(lines[...])
    total = dot(lines_high, high[...]) + (dot(lines_low, high[...]) + dot(lines_high, low[...]))
    waves = total.shape[1] // 2
    piece = waves // 2
    for x in range(along_x):
        top = total[x * 16 : x * 16 + 8]
        bottom = total[x * 16 + 8 : x * 16 + 16]
        new_real = top[:, :waves] + bottom[:, waves:]
        new_imag = bottom[:, :waves] - top[:, waves:]
        span = slice(x * 8, x * 8 + 8)
        mine[span, :piece] = jnp.where(half == 0, new_real[:, :piece], new_real[:, piece:])
        mine[span, piece:] = jnp.where(half == 0, new_imag[:, :piece], new_imag[:, piece:])
        other[span, :piece] = jnp.where(half == 0, new_real[:, piece:], new_real[:, :piece])
        other[span, piece:] = jnp.where(half == 0, new_imag[:, piece:], new_imag[:, :piece])


def along_y_sums(got, trig, cols, along_x, along_y):
    wide = WAVES // along_y
    order = np.arange(WAVES).reshape(along_y, 2, wide // 2).transpose(1, 0, 2).reshape(-1)
    cos_y, sin_y = wave_tables(WAVES, cols * along_y)
    high, low = in_two(np.concatenate([cos_y[order].T, sin_y[order].T], axis=1))
    shape = room((along_x * 8, WAVES))
    return pl.pallas_call(
        along_y_kernel,
        in_specs=[whole_vmem()] * 4,
        out_specs=[whole_vmem()] * 2,
        out_shape=[shape, shape],
        scratch_shapes=[room((along_x * 16, along_y * LANES))],
        compiler_params=limited(),
        name="along_y",
    )(kept(got.reshape(along_x, along_y, 24, cols)), kept(trig), kept(high), kept(low))


def along_x_kernel(along_x, mine, other, high, low, out):
    half = lax.axis_index(BOTH) % 2
    lines = jnp.concatenate(
        [jnp.where(half == 0, mine[...], other[...]), jnp.where(half == 0, other[...], mine[...])], axis=0
    )
    lines_high, lines_low = split_high(lines)
    total = dot(high[...], lines_high) + (dot(high[...], lines_low) + dot(low[...], lines_high))
    waves = total.shape[0] // 2
    piece = total.shape[1] // 2
    far = (
        total[:waves, :piece] + total[waves:, piece:],
        total[:waves, piece:] - total[waves:, :piece],
    )
    tall = waves // along_x
    stacks = tall // SUBLANES
    along_y = out.shape[0] // along_x
    wide = piece // along_y
    lane = spot((SUBLANES, LANES), 1)
    for x in range(along_x):
        for part in range(2):
            tiles = [far[part][x * tall + q * 8 : x * tall + q * 8 + 8] for q in range(stacks)]
            for y in range(along_y):
                block = None
                for q in range(stacks):
                    tile = moved(tiles[q], (q - y) * wide, 1)
                    block = tile if block is None else jnp.where(lane < q * wide, block, tile)
                out[x * along_y + y, part * 8 : part * 8 + 8] = block


def along_x_sums(mine, other, rows, scale, along_x, devices):
    cos_x, sin_x = wave_tables(WAVES, rows * along_x)
    table = np.concatenate([cos_x, sin_x], axis=0) * scale
    table = table.reshape(2 * WAVES, along_x, 2, 8).transpose(0, 2, 1, 3).reshape(2 * WAVES, rows * along_x)
    high, low = in_two(table)
    return pl.pallas_call(
        lambda *refs: along_x_kernel(along_x, *refs),
        in_specs=[whole_vmem()] * 4,
        out_specs=whole_vmem(),
        out_shape=pltpu.HBM((devices, 16, LANES), jnp.float32),
        compiler_params=limited(),
        name="along_x",
    )(kept(mine), kept(other), kept(high), kept(low))


def placed_kernel(got, out):
    planes, tall, wide = out.shape[1:]
    piece = wide // 2
    lane = spot((SUBLANES, LANES), 1)
    for plane in range(planes):
        for part in range(2):
            first = got[2 * plane, part * 8 : part * 8 + 8]
            second = got[2 * plane + 1, part * 8 : part * 8 + 8]
            for q in range(tall // SUBLANES):
                tile = jnp.where(lane < piece, moved(first, -q * piece, 1), moved(second, piece - q * piece, 1))
                out[part, plane, q * 8 : q * 8 + 8, :] = tile[:, :wide]


def placed_far(got, comps, freqs, tall, wide):
    far = pl.pallas_call(
        placed_kernel,
        in_specs=[whole_vmem()],
        out_specs=whole_vmem(),
        out_shape=jax.ShapeDtypeStruct((2, comps * freqs, tall, wide), jnp.float32),
        compiler_params=limited(),
        name="placed",
    )(kept(got))
    return far.reshape(2, comps, freqs, tall, wide)


def yee_kernel(
    elec_far, magn_far, ret_far, coup_far, rows_first, rows_second, cols_first, cols_second, got, trig, known, real, imag,
    new_elec, new_magn, new_real, new_imag, elec, magn, ret, coup, carried, side, arrived,
    rows_elec, rows_magn, cols_elec, cols_magn,
):
    step = pl.program_id(0)
    steps = pl.num_programs(0)
    rows, cols = ret.shape[:2]
    deep = new_elec.shape[1]
    at_x, at_y = lax.axis_index("gx"), lax.axis_index("gy")
    along_x, along_y = lax.axis_size("gx"), lax.axis_size("gy")
    here = lax.axis_index(BOTH)
    up = jnp.minimum(here + along_y - 1, along_x * along_y - 1)
    down = jnp.maximum(here - along_y + 1, 0)
    inner_x = jnp.where(at_x > 0, 1.0, 0.0)
    inner_y = jnp.where(at_y > 0, 1.0, 0.0)
    corner_up = got[pl.ds(up, 1), 21, :] * jnp.where((at_x + 1 < along_x) & (at_y > 0), curl_step, 0.0)
    corner_down = got[pl.ds(down, 1), 22, :] * jnp.where((at_x > 0) & (at_y + 1 < along_y), curl_step, 0.0)
    row = spot((LANES, LANES), 0)
    lane = spot((LANES, LANES), 1)
    chunks = arrived.shape[0]
    thick = rows // chunks
    front = SUBLANES

    def copies(chunk):
        return arrivals(
            chunk, thick, (elec_far, magn_far, ret_far, coup_far), (elec.at[:, :, 0:cols], magn, ret, coup), arrived
        )

    @pl.when(step == 0)
    def _():
        for chunk in range(chunks):
            for copy in copies(chunk):
                copy.start()
        even = at_x % 2 == 0
        rows_elec[...] = jnp.where(even, rows_first[...], rows_second[...])
        rows_magn[...] = jnp.where(even, rows_second[...], rows_first[...])
        even = at_y % 2 == 0
        cols_elec[...] = jnp.where(even, cols_first[...], cols_second[...])
        cols_magn[...] = jnp.where(even, cols_second[...], cols_first[...])
        for at in range(rows):
            elec[0, at, cols : cols + 1, :] = cols_elec[0, at : at + 1, :]
            elec[2, at, cols : cols + 1, :] = cols_elec[1, at : at + 1, :]

        lines = None
        for which, (value, plane) in enumerate(((rows_elec[0], 0), (rows_elec[1], 0), (rows_elec[1], -1), (rows_magn[1], 0))):
            turned = moved(value, which - TOP_PLANE - plane, 1)
            lines = turned if lines is None else jnp.where(lane < which, lines, turned)
        lines = lines.T
        ey_row, ez_row, ez_row_below, hz_row = (lines[which : which + 1] for which in range(4))
        ey_row, ez_row, ez_row_below = curl_step * ey_row, curl_step * ez_row, curl_step * ez_row_below
        tall = spot((rows, LANES), 0)
        wide = spot((rows, LANES), 1)
        end = LANES - 1

        def at_right(value, plane=0):
            return jnp.where(wide == end, moved(value, end - TOP_PLANE - plane, 1), 0.0)

        def at_left(value):
            return jnp.where(wide == 0, moved(value, -TOP_PLANE, 1), 0.0)

        ex_right = curl_step * at_right(cols_elec[0])
        ez_right = curl_step * at_right(cols_elec[1])
        ez_right_below = curl_step * at_right(cols_elec[1], -1)
        corner_left = jnp.where(wide[0:1] == 0, moved(corner_up, -TOP_PLANE, 1), 0.0)
        corner_right = jnp.where(wide[0:1] == end, moved(corner_down, end - TOP_PLANE, 1), 0.0)
        ey_row_left = before(ey_row, 1) + corner_left
        gain = known[4]
        push_x = ex_right - at_left(cols_magn[1]) * inner_y
        push_x = push_x + jnp.where(tall == rows - 1, ey_row_left - ey_row - (ez_row - ez_row_below), 0.0)
        push_y = before(ex_right, 0) - ex_right - (ez_right - ez_right_below)
        push_y = push_y + jnp.where(tall == rows - 1, ey_row, 0.0)
        push_y = push_y + jnp.where(tall == 0, hz_row * inner_x + corner_right, 0.0)
        tangents = (
            known[0] + gain * push_x,
            known[1] + gain * push_y,
            known[2] - ez_right,
            known[3] + jnp.where(tall == rows - 1, ez_row, 0.0),
        )
        for comp, tangent in enumerate(tangents):
            for freq in range(real.shape[1]):
                new_real[comp, freq] = real[comp, freq] + tangent * trig[0, freq : freq + 1, :]
                new_imag[comp, freq] = imag[comp, freq] - tangent * trig[1, freq : freq + 1, :]

        for copy in copies(0):
            copy.wait()
        spare = jnp.where(row == cols - 1, corner_down, 0.0)
        carried[0] = (rows_magn[0] + curl_step * elec[2, 0, 0:cols]) * inner_x
        carried[1] = (rows_magn[1] - curl_step * elec[1, 0, 0:cols] + spare) * inner_x

    ahead = (step + 1) * deep

    @pl.when((ahead % thick == 0) & (ahead < rows))
    def _():
        for copy in copies(ahead // thick):
            copy.wait()

    at_end = step == steps - 1
    for inner in range(deep):
        at = step * deep + inner
        line = pl.ds(at, 1)
        ex, ey, ez = elec[0, at, 0:cols], elec[1, at, 0:cols], elec[2, at, 0:cols]
        if inner + 1 < deep:
            ey_next, ez_next = elec[1, at + 1, 0:cols], elec[2, at + 1, 0:cols]
        else:
            then = jnp.minimum(at + 1, rows - 1)
            ey_next = jnp.where(at_end, rows_elec[0], elec[1, then, 0:cols])
            ez_next = jnp.where(at_end, rows_elec[1], elec[2, then, 0:cols])
        hx = magn[0, at] - curl_step * ((elec[2, at, 1 : cols + 1] - ez) - (after(ey, 1) - ey))
        hy = magn[1, at] - curl_step * ((after(ex, 1) - ex) - (ez_next - ez))
        hz = magn[2, at] - curl_step * ((ey_next - ey) - (elec[0, at, 1 : cols + 1] - ex))
        new_magn[0, inner] = hx
        new_magn[1, inner] = hy
        new_magn[2, inner] = hz
        side_x = (cols_magn[0, line, :] - curl_step * ez[0:1]) * inner_y
        side_z = cols_magn[1, line, :] + curl_step * ex[0:1]
        if inner + 1 == deep:
            side_z = side_z - jnp.where(at_end, corner_up, 0.0)
        side[0, front - 1 : front, :] = side_x
        side[1, front - 1 : front, :] = side_z * inner_y
        side[0, front : front + cols, :] = hx
        side[1, front : front + cols, :] = hz
        hx_before, hz_before = side[0, front - 1 : front + cols - 1, :], side[1, front - 1 : front + cols - 1, :]
        keep, gain = ret[at], coup[at]
        new_elec[0, inner] = keep * ex + gain * ((hz - hz_before) - (hy - before(hy, 1)))
        new_elec[1, inner] = keep * ey + gain * ((hx - before(hx, 1)) - (hz - carried[1]))
        new_elec[2, inner] = keep * ez + gain * ((hy - carried[0]) - (hx - hx_before))
        carried[0] = hy
        carried[1] = hz


def yee(fields, halos, got, trig, known, spectrum_real, spectrum_imag):
    _, rows, cols, deep = fields[0].shape
    slab, chunks = 2, 4
    vector = pl.BlockSpec((3, slab, cols, deep), lambda i: (0, i, 0, 0))
    kind = jnp.float32
    return pl.pallas_call(
        yee_kernel,
        grid=(rows // slab,),
        in_specs=[pl.BlockSpec(memory_space=pl.ANY)] * 4 + [whole_vmem()] * 9,
        compiler_params=limited(32),
        out_specs=[vector, vector, whole_vmem(), whole_vmem()],
        out_shape=[
            jax.ShapeDtypeStruct(fields[0].shape, kind),
            jax.ShapeDtypeStruct(fields[1].shape, kind),
            jax.ShapeDtypeStruct(spectrum_real.shape, kind),
            jax.ShapeDtypeStruct(spectrum_imag.shape, kind),
        ],
        scratch_shapes=[
            room((3, rows, cols + SUBLANES, deep)),
            *(room(field.shape) for field in fields[1:]),
            room((2, cols, deep)),
            room((2, cols + SUBLANES, deep)),
            pltpu.SemaphoreType.DMA((chunks, 8)),
            room((2, cols, deep)),
            room((2, cols, deep)),
            room((2, rows, deep)),
            room((2, rows, deep)),
        ],
        cost_estimate=pl.CostEstimate(flops=60 * fields[0].size, bytes_accessed=8 * fields[0].size, transcendentals=0),
        name="yee",
    )(
        *(far_kept(field) for field in fields), *(kept(value) for value in (*halos, got, trig, known)),
        far_kept(spectrum_real), far_kept(spectrum_imag),
    )


def tiled_step(electric, magnetic, retention, coupling, spectrum_real, spectrum_imag, phases):
    comps, freqs, rows, cols = spectrum_real.shape
    along_x, along_y = lax.axis_size("gx"), lax.axis_size("gy")
    devices = along_x * along_y
    sent, rows_first, rows_second, cols_first, cols_second, trig, known = spread(
        electric, magnetic, retention, coupling, spectrum_real, spectrum_imag, phases
    )
    got = lax.all_to_all(sent, BOTH, split_axis=0, concat_axis=0, tiled=True)
    rows_traded = (traded(rows_first, "gx", 0), traded(rows_second, "gx", 1))
    halos = (*rows_traded, traded(cols_first, "gy", 0), traded(cols_second, "gy", 1))
    mine, other = along_y_sums(got, trig, cols, along_x, along_y)
    other = swapped(other, 1)
    scale = 1.0 / math.sqrt(rows * along_x * cols * along_y)
    far = along_x_sums(mine, other, rows, scale, along_x, devices)
    far = lax.all_to_all(far, BOTH, split_axis=0, concat_axis=0, tiled=True)
    next_electric, next_magnetic, next_real, next_imag = yee(
        (electric, magnetic, retention, coupling), halos, got, trig, known, spectrum_real, spectrum_imag
    )
    far_field = placed_far(far, comps, freqs, WAVES // along_x, WAVES // along_y)
    return (next_electric, next_magnetic, next_real, next_imag, far_field)


def per_device(*arrays):
    comps, freqs, rows, cols = arrays[4].shape
    depth = arrays[0].shape[3]
    along_x, along_y = lax.axis_size("gx"), lax.axis_size("gy")
    wide, tall = WAVES // along_y, WAVES // along_x
    fits = (
        comps == 4
        and along_x * along_y == 2 * comps * freqs
        and (rows, cols, depth) == (2 * SUBLANES, LANES, LANES)
        and WAVES == 2 * LANES
        and (wide // 2) * (tall // SUBLANES) == LANES
        and 0 < TOP_PLANE < depth - 1
    )
    return tiled_step(*arrays) if fits else general_step(*arrays)


def solution(mesh):
    placed = (
        P(None, "gx", "gy", None),
        P(None, "gx", "gy", None),
        P("gx", "gy", None),
        P("gx", "gy", None),
        P(None, None, "gx", "gy"),
        P(None, None, "gx", "gy"),
        P(),
    )
    return jax.shard_map(
        per_device,
        mesh=mesh,
        in_specs=placed,
        out_specs=(
            P(None, "gx", "gy", None),
            P(None, "gx", "gy", None),
            P(None, None, "gx", "gy"),
            P(None, None, "gx", "gy"),
            P(None, None, None, "gx", "gy"),
        ),
        check_vma=False,
    )
```

```python
import math

import jax
import jax.numpy as jnp
import numpy as np
from jax import lax
from jax.experimental import pallas as pl
from jax.experimental.pallas import tpu as pltpu
from jax.sharding import PartitionSpec as P


WAVES = 256
TOP_PLANE = 111
BOTH = ("gx", "gy")
LANES = 128
SUBLANES = 8
SLABS = ((0, 4), (4, 4), (8, 4), (12, 2), (14, 2))

curl_step = 0.5


def passed_along(value, axis, by):
    devices = lax.axis_size(axis)
    pairs = [(i, i + by) for i in range(devices) if 0 <= i + by < devices]
    return lax.ppermute(value, axis, pairs)


def traded(value, axis, odd):
    devices = lax.axis_size(axis)
    pairs = [(i, i + 1 if i % 2 == odd else i - 1) for i in range(devices)]
    return lax.ppermute(value, axis, [(i, to) for i, to in pairs if 0 <= to < devices])


def swapped(value, by):
    devices = lax.axis_size(BOTH)
    return lax.ppermute(value, BOTH, [(i, i ^ by) for i in range(devices)])


def wave_tables(number, extent):
    wave = 2 * np.arange(number) + 1 - number
    angles = (wave[:, None] * np.arange(extent)[None, :] % (4 * number)) * (math.pi / (2 * number))
    return np.cos(angles), np.sin(angles)


def in_two(table):
    high = table.astype(np.float32).astype(jnp.bfloat16)
    low = (table - high.astype(np.float64)).astype(np.float32).astype(jnp.bfloat16)
    return jnp.asarray(high), jnp.asarray(low)


def forward_diff(values, along):
    padded = jnp.pad(values, [(0, 1) if which == along else (0, 0) for which in range(values.ndim)])
    return lax.slice_in_dim(padded, 1, values.shape[along] + 1, axis=along) - values


def backward_diff(values, along):
    padded = jnp.pad(values, [(1, 0) if which == along else (0, 0) for which in range(values.ndim)])
    return values - lax.slice_in_dim(padded, 0, values.shape[along], axis=along)


def ahead_diff(values, border, along):
    upper = lax.slice_in_dim(values, 1, values.shape[along], axis=along)
    return jnp.concatenate([upper, border], axis=along) - values


def behind_diff(values, border, along):
    lower = lax.slice_in_dim(values, 0, values.shape[along] - 1, axis=along)
    return values - jnp.concatenate([border, lower], axis=along)


def far_of(next_real, next_imag):
    highest = lax.Precision.HIGHEST
    comps, freqs, rows, cols = next_real.shape
    along_x, along_y = lax.axis_size("gx"), lax.axis_size("gy")
    devices = along_x * along_y
    planes = comps * freqs
    share = devices // planes
    part_rows = rows // share
    wide = WAVES // along_y
    part_wide = wide // share
    tall = WAVES // along_x
    place = lax.axis_index(BOTH) % share

    both = jnp.stack([next_real, next_imag]).reshape(2, planes, share, part_rows, cols)
    both = both.transpose(1, 2, 0, 3, 4).reshape(devices, 2, part_rows, cols)
    got = lax.all_to_all(both, BOTH, split_axis=0, concat_axis=0, tiled=True)
    got = got.reshape(along_x, along_y, 2, part_rows, cols)

    cos_y, sin_y = (table.astype(np.float32) for table in wave_tables(WAVES, cols * along_y))
    order_k = np.arange(WAVES).reshape(along_y, share, part_wide).transpose(1, 0, 2).reshape(-1)
    cos_y = cos_y[order_k].reshape(share, -1, along_y, cols)
    sin_y = sin_y[order_k].reshape(share, -1, along_y, cols)
    with_cos = jnp.einsum("gbirc,skbc->sigrk", got, cos_y, precision=highest)
    with_sin = jnp.einsum("gbirc,skbc->sigrk", got, sin_y, precision=highest)
    partial = jnp.stack([with_cos[:, 0] + with_sin[:, 1], with_cos[:, 1] - with_sin[:, 0]], axis=1)

    pieces = []
    for by in range(share):
        piece = lax.dynamic_index_in_dim(partial, place ^ by, 0, keepdims=False)
        pieces.append(piece if by == 0 else swapped(piece, by))
    pieces = jnp.stack(pieces)
    partial = jnp.stack(
        [lax.dynamic_index_in_dim(pieces, place ^ s, 0, keepdims=False) for s in range(share)]
    )

    cos_x, sin_x = (table.astype(np.float32) for table in wave_tables(WAVES, rows * along_x))
    cos_x = cos_x.reshape(WAVES, along_x, share, part_rows)
    sin_x = sin_x.reshape(WAVES, along_x, share, part_rows)
    with_cos = jnp.einsum("jgsr,sigrk->ijk", cos_x, partial, precision=highest)
    with_sin = jnp.einsum("jgsr,sigrk->ijk", sin_x, partial, precision=highest)
    far = jnp.stack([with_cos[0] + with_sin[1], with_cos[1] - with_sin[0]])
    far = far * (1.0 / math.sqrt(rows * along_x * cols * along_y))

    far = far.reshape(2, along_x, tall, along_y, part_wide).transpose(1, 3, 0, 2, 4)
    far = far.reshape(devices, 2, tall, part_wide)
    far = lax.all_to_all(far, BOTH, split_axis=0, concat_axis=0, tiled=True)
    far = far.reshape(comps, freqs, share, 2, tall, part_wide).transpose(3, 0, 1, 4, 2, 5)
    return far.reshape(2, comps, freqs, tall, wide)


def general_step(electric, magnetic, retention, coupling, spectrum_real, spectrum_imag, phases):
    elec_x, elec_y, elec_z = (electric[0], electric[1], electric[2])
    rows_elec = passed_along(electric[1:3, 0:1], "gx", -1)
    cols_elec = passed_along(electric[0:3:2, :, 0:1], "gy", -1)
    mag_x = magnetic[0] - curl_step * (
        ahead_diff(elec_z, cols_elec[1], 1) - forward_diff(elec_y, 2)
    )
    mag_y = magnetic[1] - curl_step * (
        forward_diff(elec_x, 2) - ahead_diff(elec_z, rows_elec[1], 0)
    )
    mag_z = magnetic[2] - curl_step * (
        ahead_diff(elec_y, rows_elec[0], 0) - ahead_diff(elec_x, cols_elec[0], 1)
    )
    next_magnetic = jnp.stack([mag_x, mag_y, mag_z])
    rows_magn = passed_along(next_magnetic[1:3, -1:], "gx", 1)
    cols_magn = passed_along(next_magnetic[0:3:2, :, -1:], "gy", 1)
    new_x = retention * elec_x + coupling * (
        behind_diff(mag_z, cols_magn[1], 1) - backward_diff(mag_y, 2)
    )
    new_y = retention * elec_y + coupling * (
        backward_diff(mag_x, 2) - behind_diff(mag_z, rows_magn[1], 0)
    )
    new_z = retention * elec_z + coupling * (
        behind_diff(mag_y, rows_magn[0], 0) - behind_diff(mag_x, cols_magn[0], 1)
    )
    next_electric = jnp.stack([new_x, new_y, new_z])
    tangent = jnp.stack(
        [
            new_x[:, :, TOP_PLANE],
            new_y[:, :, TOP_PLANE],
            mag_x[:, :, TOP_PLANE],
            mag_y[:, :, TOP_PLANE],
        ]
    )
    next_real = spectrum_real + tangent[:, None] * jnp.cos(phases)[None, :, None, None]
    next_imag = spectrum_imag - tangent[:, None] * jnp.sin(phases)[None, :, None, None]
    return (next_electric, next_magnetic, next_real, next_imag, far_of(next_real, next_imag))


def spot(shape, axis):
    return lax.broadcasted_iota(jnp.int32, shape, axis)


def moved(value, by, axis):
    by = by % value.shape[axis]
    return value if by == 0 else pltpu.roll(value, by, axis)


def after(value, axis, border=0.0):
    size = value.shape[axis]
    return jnp.where(spot(value.shape, axis) == size - 1, border, moved(value, -1, axis))


def before(value, axis, border=0.0):
    return jnp.where(spot(value.shape, axis) == 0, border, moved(value, 1, axis))


def whole_vmem():
    return pl.BlockSpec(memory_space=pltpu.VMEM)


def kept(value):
    return pltpu.with_memory_space_constraint(value, pltpu.VMEM)


def far_kept(value):
    return pltpu.with_memory_space_constraint(value, pltpu.HBM)


def room(shape, dtype=jnp.float32):
    return pltpu.VMEM(shape, dtype)


def limited(size=24):
    return pltpu.CompilerParams(vmem_limit_bytes=size * 1024 * 1024)


PLACES = LANES // SUBLANES
PICKED = ((0, -1, 3), (1, -1, 3), (2, -1, 2), (3, -1, 2), (4, -1, 2), (5, 0, 1), (6, 0, 1), (7, 0, 1))


def arrivals(chunk, first, deep, sources, targets, arrived):
    span = pl.ds(first, deep)
    pairs = []
    for source, target in zip(sources, targets):
        lead = [(i, span) for i in range(source.shape[0])] if len(source.shape) == 4 else [(span,)]
        pairs += [(source.at[at], target.at[at]) for at in lead]
    return [pltpu.make_async_copy(*pair, arrived.at[chunk, i]) for i, pair in enumerate(pairs)]


def spread_kernel(
    phases_far, elec_far, magn_far, ret_far, coup_far, real_far, imag_far,
    out_far, rows_first, rows_second, cols_first, cols_second, trig, known,
    elec, magn, ret, coup, cols_elec, cols_magn, planes, ends, out, real, imag, phases, arrived, small, leaving,
):
    chunks = arrived.shape[0]
    rows = ret.shape[0]
    freqs = real.shape[1]

    def copies(chunk):
        first, count = SLABS[chunk]
        return arrivals(chunk, first, count, (elec_far, magn_far, ret_far, coup_far), (elec, magn, ret, coup), arrived)

    extras = [
        pltpu.make_async_copy(phases_far, phases, small.at[0]),
        pltpu.make_async_copy(real_far, real, small.at[1]),
        pltpu.make_async_copy(imag_far, imag, small.at[2]),
    ]
    extras[0].start()
    for chunk in range(chunks):
        for copy in copies(chunk):
            copy.start()
    extras[1].start()
    extras[2].start()
    extras[0].wait()
    turn_row = spot((SUBLANES, LANES), 0)
    angle = jnp.zeros((SUBLANES, LANES), jnp.float32)
    for freq in range(freqs):
        angle = jnp.where(turn_row == freq, phases[freq], angle)
    trig[0] = jnp.cos(angle)
    trig[1] = jnp.sin(angle)
    lane = spot((LANES, LANES), 1)

    packed = None
    for at in range(rows):
        for chunk, (first, _) in enumerate(SLABS):
            if first == at:
                for copy in copies(chunk):
                    copy.wait()
        arrays = [elec[0, at], elec[1, at], elec[2, at], magn[0, at], magn[1, at], magn[2, at], ret[at], coup[at]]
        start = at % SUBLANES * PLACES
        for which, first, count in PICKED:
            turned = moved(arrays[which], start - TOP_PLANE - first, 1)
            packed = turned if packed is None else jnp.where(lane < start, packed, turned)
            start += count
        if at % SUBLANES == SUBLANES - 1:
            planes[at // SUBLANES] = packed.T
            packed = None
        ends[0, at : at + 1, :] = elec[0, at, -1:, :]
        ends[1, at : at + 1, :] = elec[1, at, -1:, :]
        ends[2, at : at + 1, :] = magn[2, at, -1:, :]
        cols_elec[0, at : at + 1, :] = elec[0, at, 0:1, :]
        cols_elec[1, at : at + 1, :] = elec[2, at, 0:1, :]
        line = elec[1, at, -1:, :]
        cols_magn[0, at : at + 1, :] = (
            magn[0, at, -1:, :] + curl_step * elec[2, at, -1:, :] + curl_step * (after(line, 1) - line)
        )

    last = rows - 1
    ex, ey, ez = elec[0, last], elec[1, last], elec[2, last]
    upward = (elec[1, 0], elec[2, 0])
    downward = (
        magn[1, last] - curl_step * (after(ex, 1) - ex) - curl_step * ez,
        magn[2, last] + curl_step * ey + curl_step * (after(ex, 0) - ex),
    )
    even = lax.axis_index("gx") % 2 == 0
    for i in range(2):
        rows_first[i] = jnp.where(even, downward[i], upward[i])
        rows_second[i] = jnp.where(even, upward[i], downward[i])
    end_x, end_y, end_z = ends[0], ends[1], ends[2]
    cols_magn[1] = end_z - curl_step * (after(end_y, 0) - end_y) - curl_step * end_x
    even = lax.axis_index("gy") % 2 == 0
    cols_first[...] = jnp.where(even, cols_magn[...], cols_elec[...])
    cols_second[...] = jnp.where(even, cols_elec[...], cols_magn[...])
    corner_up, corner_down = elec[1, 0, -1:, :], elec[0, last, 0:1, :]

    if rows:
        ex_m, ex_p, ex_q, ey_m, ey_p, ey_q, ez_m, ez_p, hx_m, hx_p, hy_m, hy_p, hz_p, keep, gain = (
            jnp.concatenate([planes[group, pl.ds(which, SUBLANES, stride=PLACES), :] for group in range(rows // SUBLANES)])
            for which in range(15)
        )
        hx_p = hx_p - curl_step * ((after(ez_p, 1) - ez_p) - (ey_q - ey_p))
        hx_m = hx_m - curl_step * ((after(ez_m, 1) - ez_m) - (ey_p - ey_m))
        hy_p = hy_p - curl_step * ((ex_q - ex_p) - (after(ez_p, 0) - ez_p))
        hy_m = hy_m - curl_step * ((ex_p - ex_m) - (after(ez_m, 0) - ez_m))
        hz_p = hz_p - curl_step * ((after(ey_p, 0) - ey_p) - (after(ex_p, 1) - ex_p))
        edge_x = jnp.where(lax.axis_index("gx") > 0, curl_step, 0.0)
        edge_y = jnp.where(lax.axis_index("gy") > 0, curl_step, 0.0)
        tangent = (
            keep * ex_p + gain * ((hz_p - before(hz_p, 1, edge_y * ex_p)) - (hy_p - hy_m)),
            keep * ey_p + gain * ((hx_p - hx_m) - (hz_p - before(hz_p, 0, -edge_x * ey_p))),
            hx_p,
            hy_p,
        )
        for which, value in enumerate((*tangent, gain)):
            known[which] = value
        ez_jump = curl_step * (ez_p - ez_m)
        push = -curl_step * ey_p
        none = jnp.zeros_like(ex_p)
        one = jnp.ones_like(ex_p)
        row_up = (push - before(push, 1) - ez_jump, -push, none, curl_step * ez_p)
        row_down = (none, hz_p, none, none)
        col_left = (
            curl_step * ex_p,
            -ez_jump - curl_step * ex_p + before(curl_step * ex_p, 0),
            -curl_step * ez_p,
            none,
        )
        col_right = (-hz_p, none, none, none)
        wide = lax.broadcasted_iota(jnp.int32, (LANES, LANES), 1)
        tall = lax.broadcasted_iota(jnp.int32, (SUBLANES, LANES), 0)
        lanes = lax.broadcasted_iota(jnp.int32, (SUBLANES, LANES), 1)
        pad = jnp.zeros((LANES - rows, LANES), jnp.float32)

        end = LANES - 1
        block = None
        upright = ((col_left[0], 0), (col_left[1], 0), (col_left[2], 0), (col_right[0], end), (gain, end), (gain, 0))
        for which, (value, column) in enumerate(upright):
            value = moved(value, which - column, 1)
            block = value if block is None else jnp.where(wide[0:rows] < which, block, value)
        block = jnp.concatenate([block, pad], axis=0).T
        left = [block[which : which + 1] for which in range(3)]
        right, gain_end, gain_start = (moved(block[which + 2 : which + 3], which * rows, 1) for which in (1, 2, 3))
        unit = jnp.where((lanes[0:1] >= 2 * rows) & (lanes[0:1] < 4 * rows), 1.0, 0.0)
        columns = (
            left[0] + right + gain_end + gain_start
            + jnp.where(lanes[0:1] == 4 * rows, moved(-push[0:1], 4 * rows - end, 1), 0.0),
            left[1] + gain_end + gain_start
            + jnp.where(lanes[0:1] == 4 * rows, moved(curl_step * ex_p[rows - 1 :], 4 * rows, 1), 0.0),
            left[2] + unit,
            unit,
        )
        here = lax.axis_index(BOTH)
        extras[1].wait()
        extras[2].wait()
        departures = []
        for comp in range(4):
            factor = gain if comp < 2 else one
            crossing = ((row_down[comp][rows - 1 :], factor[0:1]), (row_up[comp][0:1], factor[rows - 1 :]))
            for freq in range(freqs):
                new_real = real[comp, freq] + tangent[comp] * trig[0, freq : freq + 1, :]
                new_imag = imag[comp, freq] - tangent[comp] * trig[1, freq : freq + 1, :]
                for half in range(2):
                    to = (comp * freqs + freq) * 2 + half
                    for group, value in enumerate((new_real, new_imag)):
                        out[to, 2 * group] = value[half * 8 : half * 8 + 4]
                        out[to, 2 * group + 1] = value[half * 8 + 4 : half * 8 + 8]
                    corner = jnp.where(to > here, corner_down, corner_up)
                    extra = jnp.where(tall == 0, crossing[half][0], crossing[half][1])
                    extra = jnp.where(tall < 2, extra, jnp.where(tall == 2, columns[comp], corner))
                    out[to, 4] = extra[0:4]
            span = pl.ds(comp * freqs * 2, freqs * 2)
            departures.append(pltpu.make_async_copy(out.at[span], out_far.at[span], leaving.at[comp]))
            departures[-1].start()
        for departure in departures:
            departure.wait()


def spread(electric, magnetic, retention, coupling, spectrum_real, spectrum_imag, phases):
    _, rows, cols, deep = electric.shape
    comps, freqs = spectrum_real.shape[:2]
    chunks = len(SLABS)
    sent = (comps * freqs * 2, 5, 4, cols)
    inputs = (phases, electric, magnetic, retention, coupling, spectrum_real, spectrum_imag)
    return pl.pallas_call(
        spread_kernel,
        in_specs=[pl.BlockSpec(memory_space=pl.ANY)] * 7,
        out_specs=[pl.BlockSpec(memory_space=pl.ANY)] + [whole_vmem()] * 6,
        compiler_params=limited(),
        out_shape=[
            pltpu.HBM(sent, jnp.float32),
            room((2, cols, deep)),
            room((2, cols, deep)),
            room((2, rows, deep)),
            room((2, rows, deep)),
            room((2, SUBLANES, LANES)),
            room((comps + 1, rows, cols)),
        ],
        scratch_shapes=[
            room(electric.shape),
            room(magnetic.shape),
            room(retention.shape),
            room(coupling.shape),
            room((2, rows, deep)),
            room((2, rows, deep)),
            room((rows // SUBLANES, LANES, LANES)),
            room((3, rows, LANES)),
            room(sent),
            room(spectrum_real.shape),
            room(spectrum_imag.shape),
            pltpu.SMEM((freqs,), jnp.float32),
            pltpu.SemaphoreType.DMA((chunks, 8)),
            pltpu.SemaphoreType.DMA((3,)),
            pltpu.SemaphoreType.DMA((comps,)),
        ],
        name="spread",
    )(*(far_kept(value) for value in inputs))


def split_high(value):
    high = value.astype(jnp.bfloat16)
    return high, (value - high.astype(jnp.float32)).astype(jnp.bfloat16)


def dot(a, b):
    return jnp.dot(a, b, preferred_element_type=jnp.float32)


def along_y_kernel(got, trig, high, low, mine, other, lines):
    along_x, along_y = got.shape[0], got.shape[1]
    blocks = along_x * along_y
    at = lax.axis_index(BOTH)
    half = at % 2
    freqs = got.shape[0] * got.shape[1] // 8
    freq = (at // 2) % freqs
    weight_real = trig[0, pl.ds(freq, 1), :]
    weight_imag = -trig[1, pl.ds(freq, 1), :]

    packed = jnp.concatenate([got[x, :, 4, 2, :] for x in range(along_x)], axis=0)
    block = spot((blocks, LANES), 0)
    lane = spot((blocks, LANES), 1)
    inner = block % along_y
    rows = 16

    def lines_at(value, which):
        return jnp.where(lane < rows, moved(value, -which * rows, 1), 0.0)

    from_right = jnp.where(inner == along_y - 1, 0.0, moved(packed, -1, 0))
    from_left = jnp.where(inner == 0, 0.0, moved(packed, 1, 0))
    comp = at // (2 * freqs)
    right_up = jnp.where((block >= along_y) & (comp == 1), moved(from_right, along_y, 0), 0.0)
    left_down = jnp.where((block < blocks - along_y) & (comp == 0), moved(from_left, -along_y, 0), 0.0)
    from_right = lines_at(from_right, 0) + jnp.where(lane == 0, moved(right_up, -4 * rows, 1), 0.0)
    from_left = lines_at(from_left, 1) + jnp.where(lane == rows - 1, moved(left_down, -3 * rows - 1, 1), 0.0)
    last_col = lines_at(packed, 2) * from_right
    first_col = lines_at(packed, 3) * from_left
    pad = jnp.zeros((LANES - 2 * blocks, LANES), jnp.float32)
    upright = jnp.concatenate([last_col, first_col, pad], axis=0).T
    cols = jnp.where(half == 0, upright[0:8], upright[8:16])

    low_row = spot((SUBLANES, LANES), 0)
    low_lane = spot((SUBLANES, LANES), 1)
    crossed = jnp.where(half == 1, SUBLANES - 1, 0)
    for x in range(along_x):
        for y in range(along_y):
            here = x * along_y + y
            delta = jnp.where(low_lane == LANES - 1, moved(cols, LANES - 1 - here, 1), 0.0)
            delta = delta + jnp.where(low_lane == 0, moved(cols, -blocks - here, 1), 0.0)
            from_next = got[x + 1, y, 4, 0:1, :] if x + 1 < along_x else 0.0
            from_last = got[x - 1, y, 4, 0:1, :] if x > 0 else 0.0
            row = got[x, y, 4, 1:2, :] * jnp.where(half == 1, from_next, from_last)
            delta = delta + jnp.where(low_row == crossed, row, 0.0)
            span = slice(y * LANES, (y + 1) * LANES)
            for group, weight in enumerate((weight_real, weight_imag)):
                own = jnp.concatenate([got[x, y, 2 * group], got[x, y, 2 * group + 1]], axis=0)
                lines[x * 16 + group * 8 : x * 16 + group * 8 + 8, span] = own + weight * delta

    lines_high, lines_low = split_high(lines[...])
    total = dot(lines_high, high[...]) + (dot(lines_low, high[...]) + dot(lines_high, low[...]))
    waves = total.shape[1] // 2
    piece = waves // 2
    for x in range(along_x):
        top = total[x * 16 : x * 16 + 8]
        bottom = total[x * 16 + 8 : x * 16 + 16]
        new_real = top[:, :waves] + bottom[:, waves:]
        new_imag = bottom[:, :waves] - top[:, waves:]
        span = slice(x * 8, x * 8 + 8)
        mine[span, :piece] = jnp.where(half == 0, new_real[:, :piece], new_real[:, piece:])
        mine[span, piece:] = jnp.where(half == 0, new_imag[:, :piece], new_imag[:, piece:])
        other[span, :piece] = jnp.where(half == 0, new_real[:, piece:], new_real[:, :piece])
        other[span, piece:] = jnp.where(half == 0, new_imag[:, piece:], new_imag[:, :piece])


def along_y_sums(got, trig, cols, along_x, along_y):
    wide = WAVES // along_y
    order = np.arange(WAVES).reshape(along_y, 2, wide // 2).transpose(1, 0, 2).reshape(-1)
    cos_y, sin_y = wave_tables(WAVES, cols * along_y)
    high, low = in_two(np.concatenate([cos_y[order].T, sin_y[order].T], axis=1))
    shape = room((along_x * 8, WAVES))
    return pl.pallas_call(
        along_y_kernel,
        in_specs=[whole_vmem()] * 4,
        out_specs=[whole_vmem()] * 2,
        out_shape=[shape, shape],
        scratch_shapes=[room((along_x * 16, along_y * LANES))],
        compiler_params=limited(),
        name="along_y",
    )(kept(got.reshape(along_x, along_y, *got.shape[1:])), kept(trig), kept(high), kept(low))


def along_x_kernel(along_x, mine, other, high, low, out):
    half = lax.axis_index(BOTH) % 2
    lines = jnp.concatenate(
        [jnp.where(half == 0, mine[...], other[...]), jnp.where(half == 0, other[...], mine[...])], axis=0
    )
    lines_high, lines_low = split_high(lines)
    total = dot(high[...], lines_high) + (dot(high[...], lines_low) + dot(low[...], lines_high))
    waves = total.shape[0] // 2
    piece = total.shape[1] // 2
    far = (
        total[:waves, :piece] + total[waves:, piece:],
        total[:waves, piece:] - total[waves:, :piece],
    )
    tall = waves // along_x
    stacks = tall // SUBLANES
    along_y = out.shape[0] // along_x
    wide = piece // along_y
    lane = spot((SUBLANES, LANES), 1)
    for x in range(along_x):
        for part in range(2):
            tiles = [far[part][x * tall + q * 8 : x * tall + q * 8 + 8] for q in range(stacks)]
            for y in range(along_y):
                block = None
                for q in range(stacks):
                    tile = moved(tiles[q], (q - y) * wide, 1)
                    block = tile if block is None else jnp.where(lane < q * wide, block, tile)
                out[x * along_y + y, part * 8 : part * 8 + 8] = block


def along_x_sums(mine, other, rows, scale, along_x, devices):
    cos_x, sin_x = wave_tables(WAVES, rows * along_x)
    table = np.concatenate([cos_x, sin_x], axis=0) * scale
    table = table.reshape(2 * WAVES, along_x, 2, 8).transpose(0, 2, 1, 3).reshape(2 * WAVES, rows * along_x)
    high, low = in_two(table)
    return pl.pallas_call(
        lambda *refs: along_x_kernel(along_x, *refs),
        in_specs=[whole_vmem()] * 4,
        out_specs=whole_vmem(),
        out_shape=pltpu.HBM((devices, 16, LANES), jnp.float32),
        compiler_params=limited(),
        name="along_x",
    )(kept(mine), kept(other), kept(high), kept(low))


def placed_kernel(got, out):
    planes, tall, wide = out.shape[1:]
    piece = wide // 2
    lane = spot((SUBLANES, LANES), 1)
    for plane in range(planes):
        for part in range(2):
            first = got[2 * plane, part * 8 : part * 8 + 8]
            second = got[2 * plane + 1, part * 8 : part * 8 + 8]
            for q in range(tall // SUBLANES):
                tile = jnp.where(lane < piece, moved(first, -q * piece, 1), moved(second, piece - q * piece, 1))
                out[part, plane, q * 8 : q * 8 + 8, :] = tile[:, :wide]


def placed_far(got, comps, freqs, tall, wide):
    far = pl.pallas_call(
        placed_kernel,
        in_specs=[whole_vmem()],
        out_specs=whole_vmem(),
        out_shape=jax.ShapeDtypeStruct((2, comps * freqs, tall, wide), jnp.float32),
        compiler_params=limited(),
        name="placed",
    )(kept(got))
    return far.reshape(2, comps, freqs, tall, wide)


def yee_kernel(
    elec_far, magn_far, ret_far, coup_far, rows_first, rows_second, cols_first, cols_second, got, trig, known, real, imag,
    new_elec, new_magn, new_real, new_imag, elec, magn, ret, coup, carried, side, arrived,
    rows_elec, rows_magn, cols_elec, cols_magn,
):
    step = pl.program_id(0)
    steps = pl.num_programs(0)
    rows, cols = ret.shape[:2]
    deep = new_elec.shape[1]
    at_x, at_y = lax.axis_index("gx"), lax.axis_index("gy")
    along_x, along_y = lax.axis_size("gx"), lax.axis_size("gy")
    here = lax.axis_index(BOTH)
    up = jnp.minimum(here + along_y - 1, along_x * along_y - 1)
    down = jnp.maximum(here - along_y + 1, 0)
    inner_x = jnp.where(at_x > 0, 1.0, 0.0)
    inner_y = jnp.where(at_y > 0, 1.0, 0.0)
    corner_up = got[pl.ds(up, 1), 4, 3, :] * jnp.where((at_x + 1 < along_x) & (at_y > 0), curl_step, 0.0)
    corner_down = got[pl.ds(down, 1), 4, 3, :] * jnp.where((at_x > 0) & (at_y + 1 < along_y), curl_step, 0.0)
    row = spot((LANES, LANES), 0)
    lane = spot((LANES, LANES), 1)
    chunks = arrived.shape[0]
    thick = rows // chunks
    front = SUBLANES

    def copies(chunk):
        return arrivals(
            chunk, chunk * thick, thick, (elec_far, magn_far, ret_far, coup_far), (elec.at[:, :, 0:cols], magn, ret, coup), arrived
        )

    @pl.when(step == 0)
    def _():
        for chunk in range(chunks):
            for copy in copies(chunk):
                copy.start()
        even = at_x % 2 == 0
        rows_elec[...] = jnp.where(even, rows_first[...], rows_second[...])
        rows_magn[...] = jnp.where(even, rows_second[...], rows_first[...])
        even = at_y % 2 == 0
        cols_elec[...] = jnp.where(even, cols_first[...], cols_second[...])
        cols_magn[...] = jnp.where(even, cols_second[...], cols_first[...])
        for at in range(rows):
            elec[0, at, cols : cols + 1, :] = cols_elec[0, at : at + 1, :]
            elec[2, at, cols : cols + 1, :] = cols_elec[1, at : at + 1, :]

        lines = None
        for which, (value, plane) in enumerate(((rows_elec[0], 0), (rows_elec[1], 0), (rows_elec[1], -1), (rows_magn[1], 0))):
            turned = moved(value, which - TOP_PLANE - plane, 1)
            lines = turned if lines is None else jnp.where(lane < which, lines, turned)
        lines = lines.T
        ey_row, ez_row, ez_row_below, hz_row = (lines[which : which + 1] for which in range(4))
        ey_row, ez_row, ez_row_below = curl_step * ey_row, curl_step * ez_row, curl_step * ez_row_below
        tall = spot((rows, LANES), 0)
        wide = spot((rows, LANES), 1)
        end = LANES - 1

        def at_right(value, plane=0):
            return jnp.where(wide == end, moved(value, end - TOP_PLANE - plane, 1), 0.0)

        def at_left(value):
            return jnp.where(wide == 0, moved(value, -TOP_PLANE, 1), 0.0)

        ex_right = curl_step * at_right(cols_elec[0])
        ez_right = curl_step * at_right(cols_elec[1])
        ez_right_below = curl_step * at_right(cols_elec[1], -1)
        corner_left = jnp.where(wide[0:1] == 0, moved(corner_up, -TOP_PLANE, 1), 0.0)
        corner_right = jnp.where(wide[0:1] == end, moved(corner_down, end - TOP_PLANE, 1), 0.0)
        ey_row_left = before(ey_row, 1) + corner_left
        gain = known[4]
        push_x = ex_right - at_left(cols_magn[1]) * inner_y
        push_x = push_x + jnp.where(tall == rows - 1, ey_row_left - ey_row - (ez_row - ez_row_below), 0.0)
        push_y = before(ex_right, 0) - ex_right - (ez_right - ez_right_below)
        push_y = push_y + jnp.where(tall == rows - 1, ey_row, 0.0)
        push_y = push_y + jnp.where(tall == 0, hz_row * inner_x + corner_right, 0.0)
        tangents = (
            known[0] + gain * push_x,
            known[1] + gain * push_y,
            known[2] - ez_right,
            known[3] + jnp.where(tall == rows - 1, ez_row, 0.0),
        )
        for comp, tangent in enumerate(tangents):
            for freq in range(real.shape[1]):
                new_real[comp, freq] = real[comp, freq] + tangent * trig[0, freq : freq + 1, :]
                new_imag[comp, freq] = imag[comp, freq] - tangent * trig[1, freq : freq + 1, :]

        for copy in copies(0):
            copy.wait()
        spare = jnp.where(row == cols - 1, corner_down, 0.0)
        carried[0] = (rows_magn[0] + curl_step * elec[2, 0, 0:cols]) * inner_x
        carried[1] = (rows_magn[1] - curl_step * elec[1, 0, 0:cols] + spare) * inner_x

    ahead = (step + 1) * deep

    @pl.when((ahead % thick == 0) & (ahead < rows))
    def _():
        for copy in copies(ahead // thick):
            copy.wait()

    at_end = step == steps - 1
    for inner in range(deep):
        at = step * deep + inner
        line = pl.ds(at, 1)
        ex, ey, ez = elec[0, at, 0:cols], elec[1, at, 0:cols], elec[2, at, 0:cols]
        if inner + 1 < deep:
            ey_next, ez_next = elec[1, at + 1, 0:cols], elec[2, at + 1, 0:cols]
        else:
            then = jnp.minimum(at + 1, rows - 1)
            ey_next = jnp.where(at_end, rows_elec[0], elec[1, then, 0:cols])
            ez_next = jnp.where(at_end, rows_elec[1], elec[2, then, 0:cols])
        hx = magn[0, at] - curl_step * ((elec[2, at, 1 : cols + 1] - ez) - (after(ey, 1) - ey))
        hy = magn[1, at] - curl_step * ((after(ex, 1) - ex) - (ez_next - ez))
        hz = magn[2, at] - curl_step * ((ey_next - ey) - (elec[0, at, 1 : cols + 1] - ex))
        new_magn[0, inner] = hx
        new_magn[1, inner] = hy
        new_magn[2, inner] = hz
        side_x = (cols_magn[0, line, :] - curl_step * ez[0:1]) * inner_y
        side_z = cols_magn[1, line, :] + curl_step * ex[0:1]
        if inner + 1 == deep:
            side_z = side_z - jnp.where(at_end, corner_up, 0.0)
        side[0, front - 1 : front, :] = side_x
        side[1, front - 1 : front, :] = side_z * inner_y
        side[0, front : front + cols, :] = hx
        side[1, front : front + cols, :] = hz
        hx_before, hz_before = side[0, front - 1 : front + cols - 1, :], side[1, front - 1 : front + cols - 1, :]
        keep, gain = ret[at], coup[at]
        new_elec[0, inner] = keep * ex + gain * ((hz - hz_before) - (hy - before(hy, 1)))
        new_elec[1, inner] = keep * ey + gain * ((hx - before(hx, 1)) - (hz - carried[1]))
        new_elec[2, inner] = keep * ez + gain * ((hy - carried[0]) - (hx - hx_before))
        carried[0] = hy
        carried[1] = hz


def yee(fields, halos, got, trig, known, spectrum_real, spectrum_imag):
    _, rows, cols, deep = fields[0].shape
    slab, chunks = 2, 4
    vector = pl.BlockSpec((3, slab, cols, deep), lambda i: (0, i, 0, 0))
    kind = jnp.float32
    return pl.pallas_call(
        yee_kernel,
        grid=(rows // slab,),
        in_specs=[pl.BlockSpec(memory_space=pl.ANY)] * 4 + [whole_vmem()] * 9,
        compiler_params=limited(32),
        out_specs=[vector, vector, whole_vmem(), whole_vmem()],
        out_shape=[
            jax.ShapeDtypeStruct(fields[0].shape, kind),
            jax.ShapeDtypeStruct(fields[1].shape, kind),
            jax.ShapeDtypeStruct(spectrum_real.shape, kind),
            jax.ShapeDtypeStruct(spectrum_imag.shape, kind),
        ],
        scratch_shapes=[
            room((3, rows, cols + SUBLANES, deep)),
            *(room(field.shape) for field in fields[1:]),
            room((2, cols, deep)),
            room((2, cols + SUBLANES, deep)),
            pltpu.SemaphoreType.DMA((chunks, 8)),
            room((2, cols, deep)),
            room((2, cols, deep)),
            room((2, rows, deep)),
            room((2, rows, deep)),
        ],
        cost_estimate=pl.CostEstimate(flops=60 * fields[0].size, bytes_accessed=8 * fields[0].size, transcendentals=0),
        name="yee",
    )(
        *(far_kept(field) for field in fields), *(kept(value) for value in (*halos, got, trig, known)),
        far_kept(spectrum_real), far_kept(spectrum_imag),
    )


def tiled_step(electric, magnetic, retention, coupling, spectrum_real, spectrum_imag, phases):
    comps, freqs, rows, cols = spectrum_real.shape
    along_x, along_y = lax.axis_size("gx"), lax.axis_size("gy")
    devices = along_x * along_y
    sent, rows_first, rows_second, cols_first, cols_second, trig, known = spread(
        electric, magnetic, retention, coupling, spectrum_real, spectrum_imag, phases
    )
    got = lax.all_to_all(sent, BOTH, split_axis=0, concat_axis=0, tiled=True)
    rows_traded = (traded(rows_first, "gx", 0), traded(rows_second, "gx", 1))
    halos = (*rows_traded, traded(cols_first, "gy", 0), traded(cols_second, "gy", 1))
    mine, other = along_y_sums(got, trig, cols, along_x, along_y)
    other = swapped(other, 1)
    scale = 1.0 / math.sqrt(rows * along_x * cols * along_y)
    far = along_x_sums(mine, other, rows, scale, along_x, devices)
    far = lax.all_to_all(far, BOTH, split_axis=0, concat_axis=0, tiled=True)
    next_electric, next_magnetic, next_real, next_imag = yee(
        (electric, magnetic, retention, coupling), halos, got, trig, known, spectrum_real, spectrum_imag
    )
    far_field = placed_far(far, comps, freqs, WAVES // along_x, WAVES // along_y)
    return (next_electric, next_magnetic, next_real, next_imag, far_field)


def per_device(*arrays):
    comps, freqs, rows, cols = arrays[4].shape
    depth = arrays[0].shape[3]
    along_x, along_y = lax.axis_size("gx"), lax.axis_size("gy")
    wide, tall = WAVES // along_y, WAVES // along_x
    fits = (
        comps == 4
        and along_x * along_y == 2 * comps * freqs
        and (rows, cols, depth) == (2 * SUBLANES, LANES, LANES)
        and WAVES == 2 * LANES
        and (wide // 2) * (tall // SUBLANES) == LANES
        and 0 < TOP_PLANE < depth - 1
    )
    return tiled_step(*arrays) if fits else general_step(*arrays)


def solution(mesh):
    placed = (
        P(None, "gx", "gy", None),
        P(None, "gx", "gy", None),
        P("gx", "gy", None),
        P("gx", "gy", None),
        P(None, None, "gx", "gy"),
        P(None, None, "gx", "gy"),
        P(),
    )
    return jax.shard_map(
        per_device,
        mesh=mesh,
        in_specs=placed,
        out_specs=(
            P(None, "gx", "gy", None),
            P(None, "gx", "gy", None),
            P(None, None, "gx", "gy"),
            P(None, None, "gx", "gy"),
            P(None, None, None, "gx", "gy"),
        ),
        check_vma=False,
    )
```

```python
import math

import jax
import jax.numpy as jnp
import numpy as np
from jax import lax
from jax.experimental import pallas as pl
from jax.experimental.pallas import tpu as pltpu
from jax.sharding import PartitionSpec as P


WAVES = 256
TOP_PLANE = 111
BOTH = ("gx", "gy")
LANES = 128
SUBLANES = 8
SLABS = ((0, 4), (4, 4), (8, 4), (12, 4))

curl_step = 0.5


def passed_along(value, axis, by):
    devices = lax.axis_size(axis)
    pairs = [(i, i + by) for i in range(devices) if 0 <= i + by < devices]
    return lax.ppermute(value, axis, pairs)


def traded(value, axis, odd):
    devices = lax.axis_size(axis)
    pairs = [(i, i + 1 if i % 2 == odd else i - 1) for i in range(devices)]
    return lax.ppermute(value, axis, [(i, to) for i, to in pairs if 0 <= to < devices])


def swapped(value, by):
    devices = lax.axis_size(BOTH)
    return lax.ppermute(value, BOTH, [(i, i ^ by) for i in range(devices)])


def wave_tables(number, extent):
    wave = 2 * np.arange(number) + 1 - number
    angles = (wave[:, None] * np.arange(extent)[None, :] % (4 * number)) * (math.pi / (2 * number))
    return np.cos(angles), np.sin(angles)


def in_two(table):
    high = table.astype(np.float32).astype(jnp.bfloat16)
    low = (table - high.astype(np.float64)).astype(np.float32).astype(jnp.bfloat16)
    return jnp.asarray(high), jnp.asarray(low)


def forward_diff(values, along):
    padded = jnp.pad(values, [(0, 1) if which == along else (0, 0) for which in range(values.ndim)])
    return lax.slice_in_dim(padded, 1, values.shape[along] + 1, axis=along) - values


def backward_diff(values, along):
    padded = jnp.pad(values, [(1, 0) if which == along else (0, 0) for which in range(values.ndim)])
    return values - lax.slice_in_dim(padded, 0, values.shape[along], axis=along)


def ahead_diff(values, border, along):
    upper = lax.slice_in_dim(values, 1, values.shape[along], axis=along)
    return jnp.concatenate([upper, border], axis=along) - values


def behind_diff(values, border, along):
    lower = lax.slice_in_dim(values, 0, values.shape[along] - 1, axis=along)
    return values - jnp.concatenate([border, lower], axis=along)


def far_of(next_real, next_imag):
    highest = lax.Precision.HIGHEST
    comps, freqs, rows, cols = next_real.shape
    along_x, along_y = lax.axis_size("gx"), lax.axis_size("gy")
    devices = along_x * along_y
    planes = comps * freqs
    share = devices // planes
    part_rows = rows // share
    wide = WAVES // along_y
    part_wide = wide // share
    tall = WAVES // along_x
    place = lax.axis_index(BOTH) % share

    both = jnp.stack([next_real, next_imag]).reshape(2, planes, share, part_rows, cols)
    both = both.transpose(1, 2, 0, 3, 4).reshape(devices, 2, part_rows, cols)
    got = lax.all_to_all(both, BOTH, split_axis=0, concat_axis=0, tiled=True)
    got = got.reshape(along_x, along_y, 2, part_rows, cols)

    cos_y, sin_y = (table.astype(np.float32) for table in wave_tables(WAVES, cols * along_y))
    order_k = np.arange(WAVES).reshape(along_y, share, part_wide).transpose(1, 0, 2).reshape(-1)
    cos_y = cos_y[order_k].reshape(share, -1, along_y, cols)
    sin_y = sin_y[order_k].reshape(share, -1, along_y, cols)
    with_cos = jnp.einsum("gbirc,skbc->sigrk", got, cos_y, precision=highest)
    with_sin = jnp.einsum("gbirc,skbc->sigrk", got, sin_y, precision=highest)
    partial = jnp.stack([with_cos[:, 0] + with_sin[:, 1], with_cos[:, 1] - with_sin[:, 0]], axis=1)

    pieces = []
    for by in range(share):
        piece = lax.dynamic_index_in_dim(partial, place ^ by, 0, keepdims=False)
        pieces.append(piece if by == 0 else swapped(piece, by))
    pieces = jnp.stack(pieces)
    partial = jnp.stack(
        [lax.dynamic_index_in_dim(pieces, place ^ s, 0, keepdims=False) for s in range(share)]
    )

    cos_x, sin_x = (table.astype(np.float32) for table in wave_tables(WAVES, rows * along_x))
    cos_x = cos_x.reshape(WAVES, along_x, share, part_rows)
    sin_x = sin_x.reshape(WAVES, along_x, share, part_rows)
    with_cos = jnp.einsum("jgsr,sigrk->ijk", cos_x, partial, precision=highest)
    with_sin = jnp.einsum("jgsr,sigrk->ijk", sin_x, partial, precision=highest)
    far = jnp.stack([with_cos[0] + with_sin[1], with_cos[1] - with_sin[0]])
    far = far * (1.0 / math.sqrt(rows * along_x * cols * along_y))

    far = far.reshape(2, along_x, tall, along_y, part_wide).transpose(1, 3, 0, 2, 4)
    far = far.reshape(devices, 2, tall, part_wide)
    far = lax.all_to_all(far, BOTH, split_axis=0, concat_axis=0, tiled=True)
    far = far.reshape(comps, freqs, share, 2, tall, part_wide).transpose(3, 0, 1, 4, 2, 5)
    return far.reshape(2, comps, freqs, tall, wide)


def general_step(electric, magnetic, retention, coupling, spectrum_real, spectrum_imag, phases):
    elec_x, elec_y, elec_z = (electric[0], electric[1], electric[2])
    rows_elec = passed_along(electric[1:3, 0:1], "gx", -1)
    cols_elec = passed_along(electric[0:3:2, :, 0:1], "gy", -1)
    mag_x = magnetic[0] - curl_step * (
        ahead_diff(elec_z, cols_elec[1], 1) - forward_diff(elec_y, 2)
    )
    mag_y = magnetic[1] - curl_step * (
        forward_diff(elec_x, 2) - ahead_diff(elec_z, rows_elec[1], 0)
    )
    mag_z = magnetic[2] - curl_step * (
        ahead_diff(elec_y, rows_elec[0], 0) - ahead_diff(elec_x, cols_elec[0], 1)
    )
    next_magnetic = jnp.stack([mag_x, mag_y, mag_z])
    rows_magn = passed_along(next_magnetic[1:3, -1:], "gx", 1)
    cols_magn = passed_along(next_magnetic[0:3:2, :, -1:], "gy", 1)
    new_x = retention * elec_x + coupling * (
        behind_diff(mag_z, cols_magn[1], 1) - backward_diff(mag_y, 2)
    )
    new_y = retention * elec_y + coupling * (
        backward_diff(mag_x, 2) - behind_diff(mag_z, rows_magn[1], 0)
    )
    new_z = retention * elec_z + coupling * (
        behind_diff(mag_y, rows_magn[0], 0) - behind_diff(mag_x, cols_magn[0], 1)
    )
    next_electric = jnp.stack([new_x, new_y, new_z])
    tangent = jnp.stack(
        [
            new_x[:, :, TOP_PLANE],
            new_y[:, :, TOP_PLANE],
            mag_x[:, :, TOP_PLANE],
            mag_y[:, :, TOP_PLANE],
        ]
    )
    next_real = spectrum_real + tangent[:, None] * jnp.cos(phases)[None, :, None, None]
    next_imag = spectrum_imag - tangent[:, None] * jnp.sin(phases)[None, :, None, None]
    return (next_electric, next_magnetic, next_real, next_imag, far_of(next_real, next_imag))


def spot(shape, axis):
    return lax.broadcasted_iota(jnp.int32, shape, axis)


def moved(value, by, axis):
    by = by % value.shape[axis]
    return value if by == 0 else pltpu.roll(value, by, axis)


def after(value, axis, border=0.0):
    size = value.shape[axis]
    return jnp.where(spot(value.shape, axis) == size - 1, border, moved(value, -1, axis))


def before(value, axis, border=0.0):
    return jnp.where(spot(value.shape, axis) == 0, border, moved(value, 1, axis))


def whole_vmem():
    return pl.BlockSpec(memory_space=pltpu.VMEM)


def kept(value):
    return pltpu.with_memory_space_constraint(value, pltpu.VMEM)


def far_kept(value):
    return pltpu.with_memory_space_constraint(value, pltpu.HBM)


def room(shape, dtype=jnp.float32):
    return pltpu.VMEM(shape, dtype)


def limited(size=24):
    return pltpu.CompilerParams(vmem_limit_bytes=size * 1024 * 1024)


PLACES = LANES // SUBLANES
PICKED = ((0, -1, 3), (1, -1, 3), (2, -1, 2), (3, -1, 2), (4, -1, 2), (5, 0, 1), (6, 0, 1), (7, 0, 1))


def arrivals(chunk, first, deep, sources, targets, arrived):
    span = pl.ds(first, deep)
    pairs = []
    for source, target in zip(sources, targets):
        lead = [(i, span) for i in range(source.shape[0])] if len(source.shape) == 4 else [(span,)]
        pairs += [(source.at[at], target.at[at]) for at in lead]
    return [pltpu.make_async_copy(*pair, arrived.at[chunk, i]) for i, pair in enumerate(pairs)]


def spread_kernel(
    phases_far, elec_far, magn_far, ret_far, coup_far, real_far, imag_far,
    out_far, rows_first, rows_second, cols_first, cols_second, trig, known,
    elec, magn, ret, coup, planes, out, real, imag, phases, arrived, small, leaving,
):
    chunks = arrived.shape[0]
    rows = ret.shape[0]
    freqs = real.shape[1]

    def copies(chunk):
        first, count = SLABS[chunk]
        return arrivals(chunk, first, count, (elec_far, magn_far, ret_far, coup_far), (elec, magn, ret, coup), arrived)

    extras = [
        pltpu.make_async_copy(phases_far, phases, small.at[0]),
        pltpu.make_async_copy(real_far, real, small.at[1]),
        pltpu.make_async_copy(imag_far, imag, small.at[2]),
    ]
    extras[0].start()
    for chunk in range(chunks):
        for copy in copies(chunk):
            copy.start()
    extras[1].start()
    extras[2].start()
    lane = spot((LANES, LANES), 1)

    packed = None
    for at in range(rows):
        for chunk, (first, _) in enumerate(SLABS):
            if first == at:
                for copy in copies(chunk):
                    copy.wait()
        if at == SLABS[1][0]:
            extras[0].wait()
            turn_row = spot((SUBLANES, LANES), 0)
            angle = jnp.zeros((SUBLANES, LANES), jnp.float32)
            for freq in range(freqs):
                angle = jnp.where(turn_row == freq, phases[freq], angle)
            trig[0] = jnp.cos(angle)
            trig[1] = jnp.sin(angle)
        arrays = [elec[0, at], elec[1, at], elec[2, at], magn[0, at], magn[1, at], magn[2, at], ret[at], coup[at]]
        start = at % SUBLANES * PLACES
        for which, first, count in PICKED:
            turned = moved(arrays[which], start - TOP_PLANE - first, 1)
            packed = turned if packed is None else jnp.where(lane < start, packed, turned)
            start += count
        if at % SUBLANES == SUBLANES - 1:
            planes[at // SUBLANES] = packed.T
            packed = None

    last = rows - 1
    corner_up, corner_down = elec[1, 0, -1:, :], elec[0, last, 0:1, :]

    if rows:
        ex_m, ex_p, ex_q, ey_m, ey_p, ey_q, ez_m, ez_p, hx_m, hx_p, hy_m, hy_p, hz_p, keep, gain = (
            jnp.concatenate([planes[group, pl.ds(which, SUBLANES, stride=PLACES), :] for group in range(rows // SUBLANES)])
            for which in range(15)
        )
        hx_p = hx_p - curl_step * ((after(ez_p, 1) - ez_p) - (ey_q - ey_p))
        hx_m = hx_m - curl_step * ((after(ez_m, 1) - ez_m) - (ey_p - ey_m))
        hy_p = hy_p - curl_step * ((ex_q - ex_p) - (after(ez_p, 0) - ez_p))
        hy_m = hy_m - curl_step * ((ex_p - ex_m) - (after(ez_m, 0) - ez_m))
        hz_p = hz_p - curl_step * ((after(ey_p, 0) - ey_p) - (after(ex_p, 1) - ex_p))
        edge_x = jnp.where(lax.axis_index("gx") > 0, curl_step, 0.0)
        edge_y = jnp.where(lax.axis_index("gy") > 0, curl_step, 0.0)
        tangent = (
            keep * ex_p + gain * ((hz_p - before(hz_p, 1, edge_y * ex_p)) - (hy_p - hy_m)),
            keep * ey_p + gain * ((hx_p - hx_m) - (hz_p - before(hz_p, 0, -edge_x * ey_p))),
            hx_p,
            hy_p,
        )
        ez_jump = curl_step * (ez_p - ez_m)
        push = -curl_step * ey_p
        none = jnp.zeros_like(ex_p)
        one = jnp.ones_like(ex_p)
        row_up = (push - before(push, 1) - ez_jump, -push, none, curl_step * ez_p)
        row_down = (none, hz_p, none, none)
        col_left = (
            curl_step * ex_p,
            -ez_jump - curl_step * ex_p + before(curl_step * ex_p, 0),
            -curl_step * ez_p,
            none,
        )
        col_right = (-hz_p, none, none, none)
        wide = lax.broadcasted_iota(jnp.int32, (LANES, LANES), 1)
        tall = lax.broadcasted_iota(jnp.int32, (SUBLANES, LANES), 0)
        lanes = lax.broadcasted_iota(jnp.int32, (SUBLANES, LANES), 1)
        pad = jnp.zeros((LANES - rows, LANES), jnp.float32)

        end = LANES - 1
        block = None
        upright = ((col_left[0], 0), (col_left[1], 0), (col_left[2], 0), (col_right[0], end), (gain, end), (gain, 0))
        for which, (value, column) in enumerate(upright):
            value = moved(value, which - column, 1)
            block = value if block is None else jnp.where(wide[0:rows] < which, block, value)
        block = jnp.concatenate([block, pad], axis=0).T
        left = [block[which : which + 1] for which in range(3)]
        right, gain_end, gain_start = (moved(block[which + 2 : which + 3], which * rows, 1) for which in (1, 2, 3))
        unit = jnp.where((lanes[0:1] >= 2 * rows) & (lanes[0:1] < 4 * rows), 1.0, 0.0)
        columns = (
            left[0] + right + gain_end + gain_start
            + jnp.where(lanes[0:1] == 4 * rows, moved(-push[0:1], 4 * rows - end, 1), 0.0),
            left[1] + gain_end + gain_start
            + jnp.where(lanes[0:1] == 4 * rows, moved(curl_step * ex_p[rows - 1 :], 4 * rows, 1), 0.0),
            left[2] + unit,
            unit,
        )
        here = lax.axis_index(BOTH)
        extras[1].wait()
        extras[2].wait()
        departures = []
        for comp in range(4):
            factor = gain if comp < 2 else one
            crossing = ((row_down[comp][rows - 1 :], factor[0:1]), (row_up[comp][0:1], factor[rows - 1 :]))
            for freq in range(freqs):
                new_real = real[comp, freq] + tangent[comp] * trig[0, freq : freq + 1, :]
                new_imag = imag[comp, freq] - tangent[comp] * trig[1, freq : freq + 1, :]
                for half in range(2):
                    to = (comp * freqs + freq) * 2 + half
                    for group, value in enumerate((new_real, new_imag)):
                        out[to, 2 * group] = value[half * 8 : half * 8 + 4]
                        out[to, 2 * group + 1] = value[half * 8 + 4 : half * 8 + 8]
                    corner = jnp.where(to > here, corner_down, corner_up)
                    extra = jnp.where(tall == 0, crossing[half][0], crossing[half][1])
                    extra = jnp.where(tall < 2, extra, jnp.where(tall == 2, columns[comp], corner))
                    out[to, 4] = extra[0:4]
            span = pl.ds(comp * freqs * 2, freqs * 2)
            departures.append(pltpu.make_async_copy(out.at[span], out_far.at[span], leaving.at[comp]))
            departures[-1].start()

        for which, value in enumerate((*tangent, gain)):
            known[which] = value
        first, final = 0, elec.shape[2] - 1
        ex, ey, ez = elec[0, last], elec[1, last], elec[2, last]
        upward = (elec[1, 0], elec[2, 0])
        downward = (
            magn[1, last] - curl_step * (after(ex, 1) - ex) - curl_step * ez,
            magn[2, last] + curl_step * ey + curl_step * (after(ex, 0) - ex),
        )
        even = lax.axis_index("gx") % 2 == 0
        for i in range(2):
            rows_first[i] = jnp.where(even, downward[i], upward[i])
            rows_second[i] = jnp.where(even, upward[i], downward[i])
        end_x, end_y, end_z = (elec[i, :, final, :] for i in range(3))
        leftward = (elec[0, :, first, :], elec[2, :, first, :])
        rightward = (
            magn[0, :, final, :] + curl_step * end_z + curl_step * (after(end_y, 1) - end_y),
            magn[2, :, final, :] - curl_step * (after(end_y, 0) - end_y) - curl_step * end_x,
        )
        even = lax.axis_index("gy") % 2 == 0
        for i in range(2):
            cols_first[i] = jnp.where(even, rightward[i], leftward[i])
            cols_second[i] = jnp.where(even, leftward[i], rightward[i])
        for departure in departures:
            departure.wait()


def spread(electric, magnetic, retention, coupling, spectrum_real, spectrum_imag, phases):
    _, rows, cols, deep = electric.shape
    comps, freqs = spectrum_real.shape[:2]
    chunks = len(SLABS)
    sent = (comps * freqs * 2, 5, 4, cols)
    inputs = (phases, electric, magnetic, retention, coupling, spectrum_real, spectrum_imag)
    return pl.pallas_call(
        spread_kernel,
        in_specs=[pl.BlockSpec(memory_space=pl.ANY)] * 7,
        out_specs=[pl.BlockSpec(memory_space=pl.ANY)] + [whole_vmem()] * 6,
        compiler_params=limited(),
        out_shape=[
            pltpu.HBM(sent, jnp.float32),
            room((2, cols, deep)),
            room((2, cols, deep)),
            room((2, rows, deep)),
            room((2, rows, deep)),
            room((2, SUBLANES, LANES)),
            room((comps + 1, rows, cols)),
        ],
        scratch_shapes=[
            room(electric.shape),
            room(magnetic.shape),
            room(retention.shape),
            room(coupling.shape),
            room((rows // SUBLANES, LANES, LANES)),
            room(sent),
            room(spectrum_real.shape),
            room(spectrum_imag.shape),
            pltpu.SMEM((freqs,), jnp.float32),
            pltpu.SemaphoreType.DMA((chunks, 8)),
            pltpu.SemaphoreType.DMA((3,)),
            pltpu.SemaphoreType.DMA((comps,)),
        ],
        name="spread",
    )(*(far_kept(value) for value in inputs))


def split_high(value):
    high = value.astype(jnp.bfloat16)
    return high, (value - high.astype(jnp.float32)).astype(jnp.bfloat16)


def dot(a, b):
    return jnp.dot(a, b, preferred_element_type=jnp.float32)


def along_y_kernel(got, trig, high, low, mine, other, lines):
    along_x, along_y = got.shape[0], got.shape[1]
    blocks = along_x * along_y
    at = lax.axis_index(BOTH)
    half = at % 2
    freqs = got.shape[0] * got.shape[1] // 8
    freq = (at // 2) % freqs
    weight_real = trig[0, pl.ds(freq, 1), :]
    weight_imag = -trig[1, pl.ds(freq, 1), :]

    packed = jnp.concatenate([got[x, :, 4, 2, :] for x in range(along_x)], axis=0)
    block = spot((blocks, LANES), 0)
    lane = spot((blocks, LANES), 1)
    inner = block % along_y
    rows = 16

    def lines_at(value, which):
        return jnp.where(lane < rows, moved(value, -which * rows, 1), 0.0)

    from_right = jnp.where(inner == along_y - 1, 0.0, moved(packed, -1, 0))
    from_left = jnp.where(inner == 0, 0.0, moved(packed, 1, 0))
    comp = at // (2 * freqs)
    right_up = jnp.where((block >= along_y) & (comp == 1), moved(from_right, along_y, 0), 0.0)
    left_down = jnp.where((block < blocks - along_y) & (comp == 0), moved(from_left, -along_y, 0), 0.0)
    from_right = lines_at(from_right, 0) + jnp.where(lane == 0, moved(right_up, -4 * rows, 1), 0.0)
    from_left = lines_at(from_left, 1) + jnp.where(lane == rows - 1, moved(left_down, -3 * rows - 1, 1), 0.0)
    last_col = lines_at(packed, 2) * from_right
    first_col = lines_at(packed, 3) * from_left
    pad = jnp.zeros((LANES - 2 * blocks, LANES), jnp.float32)
    upright = jnp.concatenate([last_col, first_col, pad], axis=0).T
    cols = jnp.where(half == 0, upright[0:8], upright[8:16])

    low_row = spot((SUBLANES, LANES), 0)
    low_lane = spot((SUBLANES, LANES), 1)
    crossed = jnp.where(half == 1, SUBLANES - 1, 0)
    for x in range(along_x):
        for y in range(along_y):
            here = x * along_y + y
            delta = jnp.where(low_lane == LANES - 1, moved(cols, LANES - 1 - here, 1), 0.0)
            delta = delta + jnp.where(low_lane == 0, moved(cols, -blocks - here, 1), 0.0)
            from_next = got[x + 1, y, 4, 0:1, :] if x + 1 < along_x else 0.0
            from_last = got[x - 1, y, 4, 0:1, :] if x > 0 else 0.0
            row = got[x, y, 4, 1:2, :] * jnp.where(half == 1, from_next, from_last)
            delta = delta + jnp.where(low_row == crossed, row, 0.0)
            span = slice(y * LANES, (y + 1) * LANES)
            for group, weight in enumerate((weight_real, weight_imag)):
                own = jnp.concatenate([got[x, y, 2 * group], got[x, y, 2 * group + 1]], axis=0)
                lines[x * 16 + group * 8 : x * 16 + group * 8 + 8, span] = own + weight * delta

    lines_high, lines_low = split_high(lines[...])
    total = dot(lines_high, high[...]) + (dot(lines_low, high[...]) + dot(lines_high, low[...]))
    waves = total.shape[1] // 2
    piece = waves // 2
    for x in range(along_x):
        top = total[x * 16 : x * 16 + 8]
        bottom = total[x * 16 + 8 : x * 16 + 16]
        new_real = top[:, :waves] + bottom[:, waves:]
        new_imag = bottom[:, :waves] - top[:, waves:]
        span = slice(x * 8, x * 8 + 8)
        mine[span, :piece] = jnp.where(half == 0, new_real[:, :piece], new_real[:, piece:])
        mine[span, piece:] = jnp.where(half == 0, new_imag[:, :piece], new_imag[:, piece:])
        other[span, :piece] = jnp.where(half == 0, new_real[:, piece:], new_real[:, :piece])
        other[span, piece:] = jnp.where(half == 0, new_imag[:, piece:], new_imag[:, :piece])


def along_y_sums(got, trig, cols, along_x, along_y):
    wide = WAVES // along_y
    order = np.arange(WAVES).reshape(along_y, 2, wide // 2).transpose(1, 0, 2).reshape(-1)
    cos_y, sin_y = wave_tables(WAVES, cols * along_y)
    high, low = in_two(np.concatenate([cos_y[order].T, sin_y[order].T], axis=1))
    shape = room((along_x * 8, WAVES))
    return pl.pallas_call(
        along_y_kernel,
        in_specs=[whole_vmem()] * 4,
        out_specs=[whole_vmem()] * 2,
        out_shape=[shape, shape],
        scratch_shapes=[room((along_x * 16, along_y * LANES))],
        compiler_params=limited(),
        name="along_y",
    )(kept(got.reshape(along_x, along_y, *got.shape[1:])), kept(trig), kept(high), kept(low))


def along_x_kernel(along_x, mine, other, high, low, out_far, out, leaving):
    half = lax.axis_index(BOTH) % 2
    lines = jnp.concatenate(
        [jnp.where(half == 0, mine[...], other[...]), jnp.where(half == 0, other[...], mine[...])], axis=0
    )
    lines_high, lines_low = split_high(lines)
    total = dot(high[...], lines_high) + (dot(high[...], lines_low) + dot(low[...], lines_high))
    waves = total.shape[0] // 2
    piece = total.shape[1] // 2
    far = (
        total[:waves, :piece] + total[waves:, piece:],
        total[:waves, piece:] - total[waves:, :piece],
    )
    tall = waves // along_x
    stacks = tall // SUBLANES
    along_y = out.shape[0] // along_x
    wide = piece // along_y
    lane = spot((SUBLANES, LANES), 1)
    departures = []
    for x in range(along_x):
        for part in range(2):
            tiles = [far[part][x * tall + q * 8 : x * tall + q * 8 + 8] for q in range(stacks)]
            for y in range(along_y):
                block = None
                for q in range(stacks):
                    tile = moved(tiles[q], (q - y) * wide, 1)
                    block = tile if block is None else jnp.where(lane < q * wide, block, tile)
                out[x * along_y + y, part * 8 : part * 8 + 8] = block
        span = pl.ds(x * along_y, along_y)
        departures.append(pltpu.make_async_copy(out.at[span], out_far.at[span], leaving.at[x]))
        departures[-1].start()
    for departure in departures:
        departure.wait()


def along_x_sums(mine, other, rows, scale, along_x, devices):
    cos_x, sin_x = wave_tables(WAVES, rows * along_x)
    table = np.concatenate([cos_x, sin_x], axis=0) * scale
    table = table.reshape(2 * WAVES, along_x, 2, 8).transpose(0, 2, 1, 3).reshape(2 * WAVES, rows * along_x)
    high, low = in_two(table)
    return pl.pallas_call(
        lambda *refs: along_x_kernel(along_x, *refs),
        in_specs=[whole_vmem()] * 4,
        out_specs=pl.BlockSpec(memory_space=pl.ANY),
        out_shape=pltpu.HBM((devices, 16, LANES), jnp.float32),
        scratch_shapes=[room((devices, 16, LANES)), pltpu.SemaphoreType.DMA((along_x,))],
        compiler_params=limited(),
        name="along_x",
    )(kept(mine), kept(other), kept(high), kept(low))


def placed_kernel(got, out_far, out, leaving):
    planes, tall, wide = out.shape[1:]
    parts = leaving.shape[0]
    departures = []
    piece = wide // 2
    lane = spot((SUBLANES, LANES), 1)
    for plane in range(planes):
        for part in range(2):
            first = got[2 * plane, part * 8 : part * 8 + 8]
            second = got[2 * plane + 1, part * 8 : part * 8 + 8]
            for q in range(tall // SUBLANES):
                tile = jnp.where(lane < piece, moved(first, -q * piece, 1), moved(second, piece - q * piece, 1))
                out[part, plane, q * 8 : q * 8 + 8, :] = tile[:, :wide]
        if (plane + 1) % (planes // parts) == 0:
            span = pl.ds(plane + 1 - planes // parts, planes // parts)
            at = len(departures)
            departures.append(pltpu.make_async_copy(out.at[:, span], out_far.at[:, span], leaving.at[at]))
            departures[-1].start()
    for departure in departures:
        departure.wait()


def placed_far(got, comps, freqs, tall, wide):
    far = pl.pallas_call(
        placed_kernel,
        in_specs=[whole_vmem()],
        out_specs=pl.BlockSpec(memory_space=pl.ANY),
        out_shape=jax.ShapeDtypeStruct((2, comps * freqs, tall, wide), jnp.float32),
        scratch_shapes=[room((2, comps * freqs, tall, wide)), pltpu.SemaphoreType.DMA((comps,))],
        compiler_params=limited(),
        name="placed",
    )(kept(got))
    return far.reshape(2, comps, freqs, tall, wide)


def yee_kernel(
    elec_far, magn_far, ret_far, coup_far, rows_first, rows_second, cols_first, cols_second, got, trig, known, real, imag,
    new_elec, new_magn, new_real, new_imag, elec, magn, ret, coup, carried, side, arrived,
    rows_elec, rows_magn, cols_elec, cols_magn,
):
    step = pl.program_id(0)
    steps = pl.num_programs(0)
    rows, cols = ret.shape[:2]
    deep = new_elec.shape[1]
    at_x, at_y = lax.axis_index("gx"), lax.axis_index("gy")
    along_x, along_y = lax.axis_size("gx"), lax.axis_size("gy")
    here = lax.axis_index(BOTH)
    up = jnp.minimum(here + along_y - 1, along_x * along_y - 1)
    down = jnp.maximum(here - along_y + 1, 0)
    inner_x = jnp.where(at_x > 0, 1.0, 0.0)
    inner_y = jnp.where(at_y > 0, 1.0, 0.0)
    corner_up = got[pl.ds(up, 1), 4, 3, :] * jnp.where((at_x + 1 < along_x) & (at_y > 0), curl_step, 0.0)
    corner_down = got[pl.ds(down, 1), 4, 3, :] * jnp.where((at_x > 0) & (at_y + 1 < along_y), curl_step, 0.0)
    row = spot((LANES, LANES), 0)
    lane = spot((LANES, LANES), 1)
    chunks = arrived.shape[0]
    thick = rows // chunks
    front = SUBLANES

    def copies(chunk):
        return arrivals(
            chunk, chunk * thick, thick, (elec_far, magn_far, ret_far, coup_far), (elec.at[:, :, 0:cols], magn, ret, coup), arrived
        )

    @pl.when(step == 0)
    def _():
        for chunk in range(chunks):
            for copy in copies(chunk):
                copy.start()
        even = at_x % 2 == 0
        rows_elec[...] = jnp.where(even, rows_first[...], rows_second[...])
        rows_magn[...] = jnp.where(even, rows_second[...], rows_first[...])
        even = at_y % 2 == 0
        cols_elec[...] = jnp.where(even, cols_first[...], cols_second[...])
        cols_magn[...] = jnp.where(even, cols_second[...], cols_first[...])
        for at in range(rows):
            elec[0, at, cols : cols + 1, :] = cols_elec[0, at : at + 1, :]
            elec[2, at, cols : cols + 1, :] = cols_elec[1, at : at + 1, :]

        lines = None
        for which, (value, plane) in enumerate(((rows_elec[0], 0), (rows_elec[1], 0), (rows_elec[1], -1), (rows_magn[1], 0))):
            turned = moved(value, which - TOP_PLANE - plane, 1)
            lines = turned if lines is None else jnp.where(lane < which, lines, turned)
        lines = lines.T
        ey_row, ez_row, ez_row_below, hz_row = (lines[which : which + 1] for which in range(4))
        ey_row, ez_row, ez_row_below = curl_step * ey_row, curl_step * ez_row, curl_step * ez_row_below
        tall = spot((rows, LANES), 0)
        wide = spot((rows, LANES), 1)
        end = LANES - 1

        def at_right(value, plane=0):
            return jnp.where(wide == end, moved(value, end - TOP_PLANE - plane, 1), 0.0)

        def at_left(value):
            return jnp.where(wide == 0, moved(value, -TOP_PLANE, 1), 0.0)

        ex_right = curl_step * at_right(cols_elec[0])
        ez_right = curl_step * at_right(cols_elec[1])
        ez_right_below = curl_step * at_right(cols_elec[1], -1)
        corner_left = jnp.where(wide[0:1] == 0, moved(corner_up, -TOP_PLANE, 1), 0.0)
        corner_right = jnp.where(wide[0:1] == end, moved(corner_down, end - TOP_PLANE, 1), 0.0)
        ey_row_left = before(ey_row, 1) + corner_left
        gain = known[4]
        push_x = ex_right - at_left(cols_magn[1]) * inner_y
        push_x = push_x + jnp.where(tall == rows - 1, ey_row_left - ey_row - (ez_row - ez_row_below), 0.0)
        push_y = before(ex_right, 0) - ex_right - (ez_right - ez_right_below)
        push_y = push_y + jnp.where(tall == rows - 1, ey_row, 0.0)
        push_y = push_y + jnp.where(tall == 0, hz_row * inner_x + corner_right, 0.0)
        tangents = (
            known[0] + gain * push_x,
            known[1] + gain * push_y,
            known[2] - ez_right,
            known[3] + jnp.where(tall == rows - 1, ez_row, 0.0),
        )
        for comp, tangent in enumerate(tangents):
            for freq in range(real.shape[1]):
                new_real[comp, freq] = real[comp, freq] + tangent * trig[0, freq : freq + 1, :]
                new_imag[comp, freq] = imag[comp, freq] - tangent * trig[1, freq : freq + 1, :]

        for copy in copies(0):
            copy.wait()
        spare = jnp.where(row == cols - 1, corner_down, 0.0)
        carried[0] = (rows_magn[0] + curl_step * elec[2, 0, 0:cols]) * inner_x
        carried[1] = (rows_magn[1] - curl_step * elec[1, 0, 0:cols] + spare) * inner_x

    ahead = (step + 1) * deep

    @pl.when((ahead % thick == 0) & (ahead < rows))
    def _():
        for copy in copies(ahead // thick):
            copy.wait()

    at_end = step == steps - 1
    for inner in range(deep):
        at = step * deep + inner
        line = pl.ds(at, 1)
        ex, ey, ez = elec[0, at, 0:cols], elec[1, at, 0:cols], elec[2, at, 0:cols]
        if inner + 1 < deep:
            ey_next, ez_next = elec[1, at + 1, 0:cols], elec[2, at + 1, 0:cols]
        else:
            then = jnp.minimum(at + 1, rows - 1)
            ey_next = jnp.where(at_end, rows_elec[0], elec[1, then, 0:cols])
            ez_next = jnp.where(at_end, rows_elec[1], elec[2, then, 0:cols])
        hx = magn[0, at] - curl_step * ((elec[2, at, 1 : cols + 1] - ez) - (after(ey, 1) - ey))
        hy = magn[1, at] - curl_step * ((after(ex, 1) - ex) - (ez_next - ez))
        hz = magn[2, at] - curl_step * ((ey_next - ey) - (elec[0, at, 1 : cols + 1] - ex))
        new_magn[0, inner] = hx
        new_magn[1, inner] = hy
        new_magn[2, inner] = hz
        side_x = (cols_magn[0, line, :] - curl_step * ez[0:1]) * inner_y
        side_z = cols_magn[1, line, :] + curl_step * ex[0:1]
        if inner + 1 == deep:
            side_z = side_z - jnp.where(at_end, corner_up, 0.0)
        side[0, front - 1 : front, :] = side_x
        side[1, front - 1 : front, :] = side_z * inner_y
        side[0, front : front + cols, :] = hx
        side[1, front : front + cols, :] = hz
        hx_before, hz_before = side[0, front - 1 : front + cols - 1, :], side[1, front - 1 : front + cols - 1, :]
        keep, gain = ret[at], coup[at]
        new_elec[0, inner] = keep * ex + gain * ((hz - hz_before) - (hy - before(hy, 1)))
        new_elec[1, inner] = keep * ey + gain * ((hx - before(hx, 1)) - (hz - carried[1]))
        new_elec[2, inner] = keep * ez + gain * ((hy - carried[0]) - (hx - hx_before))
        carried[0] = hy
        carried[1] = hz


def yee(fields, halos, got, trig, known, spectrum_real, spectrum_imag):
    _, rows, cols, deep = fields[0].shape
    slab, chunks = 2, 4
    vector = pl.BlockSpec((3, slab, cols, deep), lambda i: (0, i, 0, 0))
    kind = jnp.float32
    return pl.pallas_call(
        yee_kernel,
        grid=(rows // slab,),
        in_specs=[pl.BlockSpec(memory_space=pl.ANY)] * 4 + [whole_vmem()] * 9,
        compiler_params=limited(32),
        out_specs=[vector, vector, whole_vmem(), whole_vmem()],
        out_shape=[
            jax.ShapeDtypeStruct(fields[0].shape, kind),
            jax.ShapeDtypeStruct(fields[1].shape, kind),
            jax.ShapeDtypeStruct(spectrum_real.shape, kind),
            jax.ShapeDtypeStruct(spectrum_imag.shape, kind),
        ],
        scratch_shapes=[
            room((3, rows, cols + SUBLANES, deep)),
            *(room(field.shape) for field in fields[1:]),
            room((2, cols, deep)),
            room((2, cols + SUBLANES, deep)),
            pltpu.SemaphoreType.DMA((chunks, 8)),
            room((2, cols, deep)),
            room((2, cols, deep)),
            room((2, rows, deep)),
            room((2, rows, deep)),
        ],
        cost_estimate=pl.CostEstimate(flops=60 * fields[0].size, bytes_accessed=8 * fields[0].size, transcendentals=0),
        name="yee",
    )(
        *(far_kept(field) for field in fields), *(kept(value) for value in (*halos, got, trig, known)),
        far_kept(spectrum_real), far_kept(spectrum_imag),
    )


def tiled_step(electric, magnetic, retention, coupling, spectrum_real, spectrum_imag, phases):
    comps, freqs, rows, cols = spectrum_real.shape
    along_x, along_y = lax.axis_size("gx"), lax.axis_size("gy")
    devices = along_x * along_y
    sent, rows_first, rows_second, cols_first, cols_second, trig, known = spread(
        electric, magnetic, retention, coupling, spectrum_real, spectrum_imag, phases
    )
    got = lax.all_to_all(sent, BOTH, split_axis=0, concat_axis=0, tiled=True)
    rows_traded = (traded(rows_first, "gx", 0), traded(rows_second, "gx", 1))
    halos = (*rows_traded, traded(cols_first, "gy", 0), traded(cols_second, "gy", 1))
    mine, other = along_y_sums(got, trig, cols, along_x, along_y)
    other = swapped(other, 1)
    scale = 1.0 / math.sqrt(rows * along_x * cols * along_y)
    far = along_x_sums(mine, other, rows, scale, along_x, devices)
    far = lax.all_to_all(far, BOTH, split_axis=0, concat_axis=0, tiled=True)
    next_electric, next_magnetic, next_real, next_imag = yee(
        (electric, magnetic, retention, coupling), halos, got, trig, known, spectrum_real, spectrum_imag
    )
    far_field = placed_far(far, comps, freqs, WAVES // along_x, WAVES // along_y)
    return (next_electric, next_magnetic, next_real, next_imag, far_field)


def per_device(*arrays):
    comps, freqs, rows, cols = arrays[4].shape
    depth = arrays[0].shape[3]
    along_x, along_y = lax.axis_size("gx"), lax.axis_size("gy")
    wide, tall = WAVES // along_y, WAVES // along_x
    fits = (
        comps == 4
        and along_x * along_y == 2 * comps * freqs
        and (rows, cols, depth) == (2 * SUBLANES, LANES, LANES)
        and WAVES == 2 * LANES
        and (wide // 2) * (tall // SUBLANES) == LANES
        and 0 < TOP_PLANE < depth - 1
    )
    return tiled_step(*arrays) if fits else general_step(*arrays)


def solution(mesh):
    placed = (
        P(None, "gx", "gy", None),
        P(None, "gx", "gy", None),
        P("gx", "gy", None),
        P("gx", "gy", None),
        P(None, None, "gx", "gy"),
        P(None, None, "gx", "gy"),
        P(),
    )
    return jax.shard_map(
        per_device,
        mesh=mesh,
        in_specs=placed,
        out_specs=(
            P(None, "gx", "gy", None),
            P(None, "gx", "gy", None),
            P(None, None, "gx", "gy"),
            P(None, None, "gx", "gy"),
            P(None, None, None, "gx", "gy"),
        ),
        check_vma=False,
    )
```
